128 devices in a mesh: section: 2 (over z_lo), dev: 64 (over z_hi, x, y, core).
Axes of the slice: x: 4, y: 4, z: 4 (z_hi: 2, z_lo: 2; z = z_hi * 2 + z_lo), core: 2. Of those that a mesh axis runs over, the one named last changes fastest.
Arguments:
- frames: bfloat16 [2048, 32, 1024], P(('section', 'dev')), may hold values from -6 to 6
- window_counts: int32 [2, 64], replicated, may hold values from 1 to 20, 1024 in all within a row
- learned_queries: bfloat16 [32, 1024], replicated, may hold values from -6 to 6
- frame_kv: bfloat16 [1024, 2048], replicated, may hold values from -0.1875 to 0.1875
- query_out: bfloat16 [1024, 1024], replicated, may hold values from -0.1875 to 0.1875
- query_gain: float32 [1024], replicated, may hold values from 0.25 to 1.75
- captions: bfloat16 [2, 64, 128, 2048], P('section', 'dev'), may hold values from -6 to 6
- caption_lengths: int32 [2, 64], P('section', 'dev'), may hold values from 1 to 128
- caption_gain: float32 [2048], replicated, may hold values from 0.25 to 1.75
- w_query: bfloat16 [2048, 1024], replicated, may hold values from -0.125 to 0.125
- memory_kv: bfloat16 [1024, 2048], replicated, may hold values from -0.1875 to 0.1875
- w_output: bfloat16 [1024, 2048], replicated, may hold values from -0.1875 to 0.1875
- upstream: bfloat16 [2, 64, 128, 2048], P('section', 'dev'), may hold values from -6 to 6
Outputs:
- decoded: bfloat16 [2, 64, 128, 2048], P('section', 'dev')
- caption_grad: bfloat16 [2, 64, 128, 2048], P('section', 'dev')
- memory_grad: bfloat16 [2048, 32, 1024], P(('section', 'dev'))
- kv_grad: float32 [1024, 2048], P(('section', 'dev'))
The draws below stay inside these ranges and needn't reach their ends.
Inputs may be any that keep to these rules, and one draw needn't show every extreme that they name: `window_counts`: each row sums to 1024; in each row some video has exactly 20.
All inputs are finite; a program needn't handle non-finite values.
Results may differ from the reference program's by a relative error of at most 0.023.
Values may be sent and summed in bfloat16 or wider, within the bound.
No kernel may reach another device: no remote copies, remote signals or barrier semaphores. Data moves between devices by JAX's collectives and lax.ppermute only.
A program may use at most 192 MiB of HBM per device.

```python
import math
import jax
import jax.numpy as jnp
import numpy as np
from jax import lax

DMODEL = 2048
HEADS = 16
HEAD_DIM = 64
INNER = 1024
QDIM = 1024
QHEADS = 16
QUERIES = 32
FRAMES = 32
WIN_DEV = 16
MOST_WIN = 20
SLOTS = 1
CAPLEN = 128
GROUPS = 2
VIDEOS = 64
WINDOWS = 2048
N_SECTION = 2
N_DEV = 64


def place_ends(array, key, least, high):
    longest = array.shape.index(max(array.shape))
    spots = []
    for shift in (0, 1):
        where = [jax.random.randint(jax.random.fold_in(key, axis), (), 0, length) for axis, length in enumerate(array.shape)]
        where[longest] = (where[longest] + shift) % array.shape[longest]
        spots.append(tuple(where))
    return array.at[spots[0]].set(least).at[spots[1]].set(high)


def block_levels(own_key, dims, split, least, high):
    def one(dim, blocks):
        draws = jax.random.uniform(jax.random.fold_in(jax.random.fold_in(own_key, 6), dim), (blocks,), jnp.float32, least / len(split), high / len(split))
        return jnp.repeat(jnp.exp(draws), dims[dim] // blocks).reshape((-1,) + (1,) * (len(dims) - dim - 1))

    loudness = one(*split[0])
    for cut in split[1:]:
        loudness = loudness * one(*cut)
    return loudness


def profile(number_of, total, bound, slope):
    portions = [(1 << 20) // math.isqrt(rank ** slope) + 1 for rank in range(2, number_of + 1)]
    spare, given = total - bound - (number_of - 1), [1] * (number_of - 1)
    while spare > 0:
        candidates = [i for i in range(number_of - 1) if given[i] < bound]
        pool, budget = sum([portions[i] for i in candidates]), spare
        for i in candidates:
            more = min(bound - given[i], max(1, budget * portions[i] // pool), spare)
            given[i] = given[i] + more
            spare = spare - more
    return np.array([bound] + given)


def ragged(rng, number_of, total, most, lean):
    if number_of == 2:
        one = jax.random.randint(rng, (), max(1, total - most), min(most, total - 1) + 1)
        return jnp.stack([one, total - one])
    sizes = jnp.asarray(profile(number_of, total, most, lean), jnp.int32)
    couples = (number_of - 1) // 2
    giver, sink = sizes[1:1 + 2 * couples:2], sizes[2:2 + 2 * couples:2]
    room = jnp.minimum(giver - 1, most - sink)
    shifted = jax.random.randint(jax.random.fold_in(rng, 1), (couples,), 0, 1 << 20) % (room + 1)
    sizes = sizes.at[1:1 + 2 * couples:2].set(giver - shifted).at[2:2 + 2 * couples:2].set(sink + shifted)
    return sizes[jax.random.permutation(jax.random.fold_in(rng, 2), number_of)]


def normal_values(stream_key, extent, spread, most, shards=(), kind=jnp.bfloat16):
    entries = spread * jax.random.normal(stream_key, extent, jnp.float32)
    if shards:
        entries = entries * block_levels(stream_key, extent, shards, -0.22, 0.18)
    return jnp.clip(entries, -most, most).astype(kind)


def setup_inputs(seed: int = 0) -> dict:
    streams_of = jax.random.split(jax.random.key(seed), 14)
    frames = normal_values(streams_of[0], (WINDOWS, FRAMES, QDIM), 1.0, 6.0, ((0, 128),))
    window_counts = jax.vmap(lambda own: ragged(own, VIDEOS, WIN_DEV * N_DEV, MOST_WIN, 2))(jax.random.split(streams_of[1], GROUPS)).reshape((GROUPS, VIDEOS)).astype(jnp.int32)
    learned_queries = normal_values(streams_of[2], (QUERIES, QDIM), 1.0, 6.0)
    frame_kv = normal_values(streams_of[3], (QDIM, 2 * QDIM), QDIM ** -0.5, 0.1875)
    query_out = normal_values(streams_of[4], (QDIM, QDIM), QDIM ** -0.5, 0.1875)
    query_gain = jnp.clip(1.0 + 0.15 * jax.random.normal(streams_of[5], (QDIM,), jnp.float32), 0.25, 1.75)
    captions = normal_values(streams_of[6], (GROUPS, VIDEOS, CAPLEN, DMODEL), 1.0, 6.0, ((0, 2), (1, 64)))
    caption_lengths = place_ends(jax.random.randint(streams_of[7], (GROUPS, VIDEOS), 1, CAPLEN + 1), jax.random.fold_in(streams_of[7], 1), 1, CAPLEN).astype(jnp.int32)
    caption_gain = jnp.clip(1.0 + 0.15 * jax.random.normal(streams_of[8], (DMODEL,), jnp.float32), 0.25, 1.75)
    w_query = normal_values(streams_of[9], (DMODEL, INNER), DMODEL ** -0.5, 0.125)
    memory_kv = normal_values(streams_of[10], (QDIM, 2 * INNER), QDIM ** -0.5, 0.1875)
    w_output = normal_values(streams_of[11], (INNER, DMODEL), INNER ** -0.5, 0.1875)
    upstream = normal_values(streams_of[12], (GROUPS, VIDEOS, CAPLEN, DMODEL), 1.0, 6.0, ((0, 2), (1, 64)))
    return {"frames": frames, "window_counts": window_counts, "learned_queries": learned_queries, "frame_kv": frame_kv, "query_out": query_out, "query_gain": query_gain, "captions": captions, "caption_lengths": caption_lengths, "caption_gain": caption_gain, "w_query": w_query, "memory_kv": memory_kv, "w_output": w_output, "upstream": upstream}


EPSILON = 1e-06

def rms_scale(values, gain):
    return values * lax.rsqrt(lax.optimization_barrier(jnp.mean(values * values, axis=-1, keepdims=True)) + EPSILON) * gain

def compress_block(frames_block, learned_queries, frame_kv, query_out, query_gain):
    blocks = frames_block.shape[0]
    flat_frames = frames_block.reshape(blocks * FRAMES, QDIM)
    key_value = jnp.dot(flat_frames, frame_kv, preferred_element_type=jnp.float32).astype(jnp.bfloat16)
    key_heads = key_value[:, :QDIM].reshape(blocks, FRAMES, QHEADS, HEAD_DIM)
    value_heads = key_value[:, QDIM:].reshape(blocks, FRAMES, QHEADS, HEAD_DIM)
    query_heads = learned_queries.reshape(QUERIES, QHEADS, HEAD_DIM)
    scores = jnp.einsum('qhe,nfhe->nhqf', query_heads.astype(jnp.float32), key_heads.astype(jnp.float32)) * HEAD_DIM ** (-0.5)
    attention = jax.nn.softmax(scores, axis=-1).astype(jnp.bfloat16)
    context = jnp.einsum('nhqf,nfhe->nqhe', attention.astype(jnp.float32), value_heads.astype(jnp.float32)).astype(jnp.bfloat16)
    projected = jnp.dot(context.reshape(blocks * QUERIES, QDIM), query_out, preferred_element_type=jnp.float32)
    hidden = learned_queries.astype(jnp.float32)[None] + projected.reshape(blocks, QUERIES, QDIM)
    return rms_scale(hidden, query_gain).astype(jnp.bfloat16)

def attend(tokens, length, upstream, key_heads, value_heads, key_live, caption_gain, w_query, w_output):
    source = tokens.astype(jnp.float32)
    inv_rms = lax.rsqrt(lax.optimization_barrier(jnp.mean(source * source, axis=-1, keepdims=True)) + EPSILON)
    normed = (source * inv_rms * caption_gain).astype(jnp.bfloat16)
    query_heads = jnp.dot(normed, w_query, preferred_element_type=jnp.float32).astype(jnp.bfloat16).reshape(CAPLEN, HEADS, HEAD_DIM)
    scores = jnp.einsum('lhe,mhe->hlm', query_heads.astype(jnp.float32), key_heads.astype(jnp.float32)) * HEAD_DIM ** (-0.5)
    scores = jnp.where(key_live[None, None, :], scores, jnp.float32(-1e+30))
    attention = jax.nn.softmax(scores, axis=-1)
    weights = attention.astype(jnp.bfloat16)
    context = jnp.einsum('hlm,mhe->lhe', weights.astype(jnp.float32), value_heads.astype(jnp.float32)).astype(jnp.bfloat16).reshape(CAPLEN, INNER)
    decoded = (source + jnp.dot(context, w_output, preferred_element_type=jnp.float32)).astype(jnp.bfloat16)
    row_live = jnp.arange(CAPLEN, dtype=jnp.int32) < length
    grad_out = jnp.where(row_live[:, None], upstream, jnp.zeros_like(upstream))
    d_context = jnp.dot(grad_out, w_output.T, preferred_element_type=jnp.float32).astype(jnp.bfloat16).reshape(CAPLEN, HEADS, HEAD_DIM)
    d_probs = jnp.einsum('lhe,mhe->hlm', d_context.astype(jnp.float32), value_heads.astype(jnp.float32))
    d_scores = (attention * (d_probs - lax.optimization_barrier(jnp.sum(d_probs * attention, axis=-1, keepdims=True))) * HEAD_DIM ** (-0.5)).astype(jnp.bfloat16)
    d_query = jnp.einsum('hlm,mhe->lhe', d_scores.astype(jnp.float32), key_heads.astype(jnp.float32)).astype(jnp.bfloat16).reshape(CAPLEN, INNER)
    d_keys = jnp.einsum('hlm,lhe->mhe', d_scores.astype(jnp.float32), query_heads.astype(jnp.float32))
    d_values = jnp.einsum('hlm,lhe->mhe', weights.astype(jnp.float32), d_context.astype(jnp.float32))
    rows_total = key_heads.shape[0]
    d_pair = jnp.concatenate([d_keys.reshape(rows_total, INNER), d_values.reshape(rows_total, INNER)], axis=1).astype(jnp.bfloat16)
    d_scaled = jnp.dot(d_query, w_query.T, preferred_element_type=jnp.float32) * caption_gain
    caption_grad = grad_out.astype(jnp.float32) + inv_rms * (d_scaled - source * inv_rms * inv_rms * lax.optimization_barrier(jnp.mean(d_scaled * source, axis=-1, keepdims=True)))
    return (decoded, caption_grad.astype(jnp.bfloat16), d_pair)

def reference(frames, window_counts, learned_queries, frame_kv, query_out, query_gain, captions, caption_lengths, caption_gain, w_query, memory_kv, w_output, upstream):
    senders = N_SECTION * N_DEV
    memory = lax.map(lambda block: compress_block(block, learned_queries, frame_kv, query_out, query_gain), frames.reshape(senders, WIN_DEV, FRAMES, QDIM)).reshape(WINDOWS, QUERIES, QDIM)
    run_ends = jnp.cumsum(window_counts, axis=1).astype(jnp.int32)
    starts = (run_ends - window_counts).astype(jnp.int32)
    position = jnp.arange(MOST_WIN, dtype=jnp.int32)
    ranked = starts[:, :, None] + position[None, None, :]
    sender = ranked // SLOTS % N_DEV
    local_index = ranked // (SLOTS * N_DEV) * SLOTS + ranked % SLOTS
    group_index = jnp.arange(GROUPS, dtype=jnp.int32)[:, None, None]
    window_id = (group_index * N_DEV + sender) * WIN_DEV + local_index
    present = position[None, None, :] < window_counts[:, :, None]
    window_id = jnp.where(present, window_id, jnp.zeros_like(window_id)).astype(jnp.int32)
    halves = jnp.take(memory, window_id.reshape(-1), axis=0).reshape(GROUPS, VIDEOS, MOST_WIN, QUERIES, QDIM)
    halves = jnp.where(present[:, :, :, None, None], halves, jnp.zeros_like(halves))
    token_pos = jnp.arange(MOST_WIN * QUERIES, dtype=jnp.int32) // QUERIES

    def per_video(carry, inputs):
        video_halves, counts, tokens, lengths, grads = inputs
        flat_halves = video_halves.reshape(GROUPS * MOST_WIN * QUERIES, QDIM)
        key_value = jnp.dot(flat_halves, memory_kv, preferred_element_type=jnp.float32).astype(jnp.bfloat16)
        key_heads = key_value[:, :INNER].reshape(-1, HEADS, HEAD_DIM)
        value_heads = key_value[:, INNER:].reshape(-1, HEADS, HEAD_DIM)
        key_live = (token_pos[None, :] < counts[:, None]).reshape(-1)
        decoded, caption_grad, d_pair = lax.map(lambda item: attend(item[0], item[1], item[2], key_heads, value_heads, key_live, caption_gain, w_query, w_output), (tokens, lengths, grads))
        d_sum = lax.optimization_barrier(jnp.sum(d_pair.astype(jnp.float32), axis=0)).astype(jnp.bfloat16)
        d_memory = jnp.dot(d_sum, memory_kv.T, preferred_element_type=jnp.float32).astype(jnp.bfloat16)
        weight_term = jnp.dot(flat_halves.T, d_sum, preferred_element_type=jnp.float32)
        return (carry + weight_term, (decoded, caption_grad, d_memory.reshape(GROUPS, MOST_WIN, QUERIES, QDIM)))
    inputs = (jnp.moveaxis(halves, 1, 0), window_counts.T, jnp.moveaxis(captions, 1, 0), caption_lengths.T, jnp.moveaxis(upstream, 1, 0))
    kv_grad, outputs = lax.scan(per_video, jnp.zeros((QDIM, 2 * INNER), jnp.float32), inputs)
    decoded = jnp.moveaxis(outputs[0], 0, 1)
    caption_grad = jnp.moveaxis(outputs[1], 0, 1)
    d_memory = jnp.moveaxis(outputs[2], 0, 1).reshape(GROUPS * VIDEOS * MOST_WIN, QUERIES, QDIM)
    window_all = jnp.arange(WINDOWS, dtype=jnp.int32)
    group_of = window_all // (N_DEV * WIN_DEV)
    device_of = window_all // WIN_DEV % N_DEV
    slot_of = window_all % WIN_DEV
    rank_of = slot_of // SLOTS * (SLOTS * N_DEV) + device_of * SLOTS + slot_of % SLOTS
    group_ends = jnp.take(run_ends, group_of, axis=0)
    owner_video = lax.optimization_barrier(jnp.sum((group_ends <= rank_of[:, None]).astype(jnp.int32), axis=1)).astype(jnp.int32)
    owner_start = jnp.take(starts.reshape(-1), group_of * VIDEOS + owner_video)
    flat_index = ((group_of * VIDEOS + owner_video) * MOST_WIN + rank_of - owner_start).astype(jnp.int32)
    memory_grad = jnp.take(d_memory, flat_index, axis=0)
    return (decoded, caption_grad, memory_grad, kv_grad)
```

```python
import jax
import jax.numpy as jnp
from jax import lax
from jax.experimental import pallas as pl
from jax.experimental.pallas import tpu as pltpu
from jax.sharding import Mesh
from jax.sharding import PartitionSpec as P

HEADS = 16
HEAD_DIM = 64
INNER = 1024
QDIM = 1024
QHEADS = 16
QUERIES = 32
FRAMES = 32
WIN_DEV = 16
MOST_WIN = 20
CAPLEN = 128
PAIRS = HEADS // 2
ROWS = MOST_WIN * QUERIES
DEV = ("dev_0", "dev_1", "dev_2", "dev_3")
CHIP = ("dev_0", "dev_1", "dev_2")
CORE = "dev_3"
SECTION_DEV = ("section", "dev_0", "dev_1", "dev_2", "dev_3")
SWAP = [(0, 1), (1, 0)]

EPSILON = 1e-06
DEAD = -1e30


def rms_scale(values, gain):
    return values * lax.rsqrt(jnp.mean(values * values, axis=-1, keepdims=True) + EPSILON) * gain


def compress_block(frames_block, learned_queries, frame_kv, query_out, query_gain):
    blocks = frames_block.shape[0]
    flat_frames = frames_block.reshape(blocks * FRAMES, QDIM)
    key_value = jnp.dot(flat_frames, frame_kv, preferred_element_type=jnp.float32).astype(
        jnp.bfloat16
    )
    key_heads = key_value[:, :QDIM].reshape(blocks, FRAMES, QHEADS, HEAD_DIM)
    value_heads = key_value[:, QDIM:].reshape(blocks, FRAMES, QHEADS, HEAD_DIM)
    query_heads = learned_queries.reshape(QUERIES, QHEADS, HEAD_DIM)
    scores = jnp.einsum(
        "qhe,nfhe->nhqf", query_heads, key_heads, preferred_element_type=jnp.float32
    ) * HEAD_DIM ** (-0.5)
    attention = jax.nn.softmax(scores, axis=-1).astype(jnp.bfloat16)
    context = jnp.einsum(
        "nhqf,nfhe->nqhe", attention, value_heads, preferred_element_type=jnp.float32
    ).astype(jnp.bfloat16)
    projected = jnp.dot(
        context.reshape(blocks * QUERIES, QDIM), query_out, preferred_element_type=jnp.float32
    )
    hidden = learned_queries.astype(jnp.float32)[None] + projected.reshape(blocks, QUERIES, QDIM)
    return rms_scale(hidden, query_gain).astype(jnp.bfloat16)


def gather_windows(index, sources, zero_fill):
    count = index.shape[0]
    limits = []
    for source in sources:
        limits.append((limits[-1] if limits else 0) + source.shape[0])

    def kernel(index_ref, *refs):
        source_refs, out_ref, sems = refs[: len(sources)], refs[-2], refs[-1]

        def each(i, act):
            which = index_ref[i]
            low = 0
            for source_ref, high in zip(source_refs, limits):

                @pl.when((which >= low) & (which < high))
                def _():
                    act(pltpu.make_async_copy(source_ref.at[which - low], out_ref.at[i], sems.at[i]))

                low = high

        @pl.loop(0, count)
        def _(i):
            each(i, lambda copy: copy.start())
            if zero_fill:

                @pl.when(index_ref[i] < 0)
                def _():
                    out_ref[i] = jnp.zeros(out_ref.shape[1:], out_ref.dtype)

        @pl.loop(0, count)
        def _(i):
            each(i, lambda copy: copy.wait())

    inner = sources[0].shape[1:]
    size = count * inner[0] * inner[1] * 2
    return pl.pallas_call(
        kernel,
        out_shape=jax.ShapeDtypeStruct((count, *inner), sources[0].dtype),
        in_specs=[pl.BlockSpec(memory_space=pltpu.SMEM)]
        + [pl.BlockSpec(memory_space=pl.ANY)] * len(sources),
        out_specs=pl.BlockSpec(memory_space=pltpu.VMEM),
        scratch_shapes=[pltpu.SemaphoreType.DMA((count,))],
        cost_estimate=pl.CostEstimate(flops=2 * 10**9, bytes_accessed=2 * size, transcendentals=0),
        name="gather_windows",
    )(index, *sources)


NT = (((1,), (1,)), ((), ()))
TN = (((0,), (0,)), ((), ()))
NN = (((1,), (0,)), ((), ()))


def stacked(own_ref, other_ref):
    both = jnp.concatenate([own_ref[...], other_ref[...]], axis=0)
    lane = lax.broadcasted_iota(jnp.int32, both.shape, 1)
    zero = jnp.zeros_like(both)
    return jnp.concatenate(
        [jnp.where(lane < HEAD_DIM, both, zero), jnp.where(lane < HEAD_DIM, zero, both)], axis=0
    )


def dot(a, b, dims):
    return lax.dot_general(a, b, dims, preferred_element_type=jnp.float32)


def masked_scores(keys, queries, live):
    scores = dot(keys, queries, NT)
    row = lax.broadcasted_iota(jnp.int32, scores.shape, 0)
    return jnp.where(row < live, scores, DEAD)


def stats_kernel(live_ref, q_own, q_other, dc_own, dc_other, kv_ref, stats_ref):
    pair = pl.program_id(0)
    keys, values = kv_ref[:, :128], kv_ref[:, 128:]
    scores = masked_scores(keys, stacked(q_own, q_other), live_ref[0])
    top = jnp.max(scores, axis=0, keepdims=True)
    grown = jnp.exp(scores - top)
    d_probs = dot(values, stacked(dc_own, dc_other), NT)
    stats_ref[0, pl.ds(pair, 1), :] = top
    stats_ref[1, pl.ds(pair, 1), :] = jnp.sum(grown, axis=0, keepdims=True)
    stats_ref[2, pl.ds(pair, 1), :] = jnp.sum(grown * d_probs, axis=0, keepdims=True)


def heads_apart(product):
    both = 2 * CAPLEN
    rows = jnp.concatenate([product[:HEAD_DIM, :both], product[HEAD_DIM:, both:]], axis=0)
    return rows.T


def grads_kernel(
    live_ref,
    q_own,
    q_other,
    dc_own,
    dc_other,
    kv_ref,
    stats_ref,
    peer_ref,
    context_own,
    context_other,
    dq_own,
    dq_other,
    dkv_ref,
):
    pair = pl.program_id(0)
    keys, values = kv_ref[:, :128], kv_ref[:, 128:]

    def mine(which):
        return stats_ref[which, pl.ds(pair, 1), :]

    def theirs(which):
        line = peer_ref[which, pl.ds(pair, 1), :]
        parts = [line[:, 128 * k : 128 * (k + 1)] for k in (1, 0, 3, 2)]
        return jnp.concatenate(parts, axis=1)

    top_mine, top_theirs = mine(0), theirs(0)
    top = jnp.maximum(top_mine, top_theirs)
    grow_mine, grow_theirs = jnp.exp(top_mine - top), jnp.exp(top_theirs - top)
    inverse = 1.0 / (mine(1) * grow_mine + theirs(1) * grow_theirs)
    delta = (mine(2) * grow_mine + theirs(2) * grow_theirs) * inverse

    queries, d_context = stacked(q_own, q_other), stacked(dc_own, dc_other)
    scores = masked_scores(keys, queries, live_ref[0])
    probs = jnp.exp(scores - top) * inverse
    weights = probs.astype(jnp.bfloat16)
    d_probs = dot(values, d_context, NT)
    d_scores = (probs * (d_probs - delta)).astype(jnp.bfloat16)
    dkv_ref[:, :128] = dot(d_scores, queries, NN).astype(jnp.bfloat16)
    dkv_ref[:, 128:] = dot(weights, d_context, NN).astype(jnp.bfloat16)
    context = heads_apart(dot(values, weights, TN))
    context_own[...] = context[:CAPLEN]
    context_other[...] = context[CAPLEN:].astype(jnp.bfloat16)
    d_query = heads_apart(dot(keys, d_scores, TN)) * HEAD_DIM ** (-0.5)
    dq_own[...] = d_query[:CAPLEN]
    dq_other[...] = d_query[CAPLEN:].astype(jnp.bfloat16)


def attention_specs():
    tokens = pl.BlockSpec((CAPLEN, 128), lambda i: (0, i))
    return tokens, [
        pl.BlockSpec(memory_space=pltpu.SMEM),
        tokens,
        tokens,
        tokens,
        tokens,
        pl.BlockSpec((ROWS, 256), lambda i: (0, i)),
    ]


def attention_stats(live, q_own, q_other, dc_own, dc_other, key_value):
    _, in_specs = attention_specs()
    return pl.pallas_call(
        stats_kernel,
        grid=(PAIRS,),
        out_shape=jax.ShapeDtypeStruct((3, PAIRS, 4 * CAPLEN), jnp.float32),
        in_specs=in_specs,
        out_specs=pl.BlockSpec((3, PAIRS, 4 * CAPLEN), lambda i: (0, 0, 0)),
        cost_estimate=pl.CostEstimate(
            flops=5 * 10**9, bytes_accessed=4 * 10**6, transcendentals=3 * 10**6
        ),
        name="attention_stats",
    )(live, q_own, q_other, dc_own, dc_other, key_value)


def attention_grads(live, q_own, q_other, dc_own, dc_other, key_value, stats, peer):
    tokens, in_specs = attention_specs()
    whole = pl.BlockSpec((3, PAIRS, 4 * CAPLEN), lambda i: (0, 0, 0))
    wide = jax.ShapeDtypeStruct((CAPLEN, INNER), jnp.float32)
    narrow = jax.ShapeDtypeStruct((CAPLEN, INNER), jnp.bfloat16)
    return pl.pallas_call(
        grads_kernel,
        grid=(PAIRS,),
        out_shape=(
            wide,
            narrow,
            wide,
            narrow,
            jax.ShapeDtypeStruct((ROWS, 2 * INNER), jnp.bfloat16),
        ),
        in_specs=in_specs + [whole, whole],
        out_specs=(tokens, tokens, tokens, tokens, pl.BlockSpec((ROWS, 256), lambda i: (0, i))),
        cost_estimate=pl.CostEstimate(
            flops=12 * 10**9, bytes_accessed=10**7, transcendentals=3 * 10**6
        ),
        name="attention_grads",
    )(live, q_own, q_other, dc_own, dc_other, key_value, stats, peer)


def local(
    frames,
    window_counts,
    learned_queries,
    frame_kv,
    query_out,
    query_gain,
    captions,
    caption_lengths,
    caption_gain,
    w_query,
    memory_kv,
    w_output,
    upstream,
):
    videos = lax.axis_size(DEV)
    chips = videos // 2
    section_id = lax.axis_index("section")
    video_id = lax.axis_index(DEV)
    core = lax.axis_index(CORE)
    sibling = video_id + 1 - 2 * core
    counts = lax.dynamic_index_in_dim(window_counts, section_id, 0, keepdims=False)
    video = jnp.arange(videos, dtype=jnp.int32)
    ends = jnp.sum(jnp.where(video[None, :] <= video[:, None], counts[None, :], 0), axis=1)
    ranked = jnp.arange(WIN_DEV, dtype=jnp.int32) * videos + video_id
    owner_chip = jnp.sum((ends[None, :] <= ranked[:, None]).astype(jnp.int32), axis=1) // 2
    chip_slot = jnp.arange(chips, dtype=jnp.int32)
    hit = chip_slot[:, None] == owner_chip[None, :]
    window = jnp.arange(WIN_DEV, dtype=jnp.int32)
    send_index = jnp.sum(jnp.where(hit, window[None, :] + 1, 0), axis=1) - 1

    def span(which):
        count = jnp.sum(jnp.where(video == which, counts, 0))
        return count, jnp.sum(jnp.where(video < which, counts, 0))

    count_here, start_here = span(video_id)
    count_near, start_near = span(sibling)
    position = jnp.arange(MOST_WIN, dtype=jnp.int32)
    rank = start_here + position
    take_index = jnp.where(
        position < count_here, rank % videos // 2 + jnp.where(rank % 2 == core, 0, chips), -1
    )
    sender = 2 * chip_slot + core
    place_here = (sender - start_here + 16 * videos) % videos
    place_near = (sender - start_near + 16 * videos) % videos
    back_index = jnp.where(
        place_here < count_here,
        place_here,
        jnp.where(place_near < count_near, MOST_WIN + place_near, -1),
    )
    live = (count_here * QUERIES)[None]

    source = captions[0, 0].astype(jnp.float32)
    inv_rms = lax.rsqrt(jnp.mean(source * source, axis=-1, keepdims=True) + EPSILON)
    normed = (source * inv_rms * caption_gain).astype(jnp.bfloat16)
    query = jnp.dot(normed, w_query, preferred_element_type=jnp.float32).astype(jnp.bfloat16)
    query = query * jnp.bfloat16(HEAD_DIM ** (-0.5))
    row_live = jnp.arange(CAPLEN, dtype=jnp.int32) < caption_lengths[0, 0]
    grad_out = jnp.where(row_live[:, None], upstream[0, 0], jnp.zeros_like(upstream[0, 0]))
    d_context = jnp.dot(grad_out, w_output.T, preferred_element_type=jnp.float32).astype(
        jnp.bfloat16
    )
    query_other = lax.ppermute(query, "section", SWAP)
    d_context_other = lax.ppermute(d_context, "section", SWAP)
    paired_kv = (
        memory_kv.reshape(QDIM, 2, PAIRS, 128).transpose(0, 2, 1, 3).reshape(QDIM, 2 * INNER)
    )

    memory = compress_block(frames, learned_queries, frame_kv, query_out, query_gain)
    packed = gather_windows(send_index, [memory], False)
    arrived = lax.all_to_all(packed, CHIP, split_axis=0, concat_axis=0, tiled=True)
    beside = lax.ppermute(arrived, CORE, SWAP)
    half = gather_windows(take_index, [arrived, beside], True).reshape(ROWS, QDIM)
    key_value = jnp.dot(half, paired_kv, preferred_element_type=jnp.float32).astype(jnp.bfloat16)

    tokens = (live, query, query_other, d_context, d_context_other, key_value)
    stats = attention_stats(*tokens)
    peer = lax.ppermute(stats, "section", SWAP)
    context_own, context_other, dq_own, dq_other, d_sum = attention_grads(*tokens, stats, peer)

    d_memory = lax.dot_general(d_sum, paired_kv, NT, preferred_element_type=jnp.float32).astype(
        jnp.bfloat16
    )
    d_memory = d_memory.reshape(MOST_WIN, QUERIES, QDIM)
    d_beside = lax.ppermute(d_memory, CORE, SWAP)
    d_packed = gather_windows(back_index, [d_memory, d_beside], False)
    returned = lax.all_to_all(d_packed, CHIP, split_axis=0, concat_axis=0, tiled=True)
    memory_grad = gather_windows(owner_chip, [returned], False)

    term = jnp.dot(half.T, d_sum, preferred_element_type=jnp.float32).astype(jnp.bfloat16)
    term = term.reshape(2 * chips, 2, QDIM // (4 * chips), 2 * INNER)
    kept = lax.dynamic_index_in_dim(term, core, 1, keepdims=False)
    given = lax.dynamic_index_in_dim(term, 1 - core, 1, keepdims=False)
    got = lax.ppermute(given, CORE, SWAP)
    chip_term = (kept.astype(jnp.float32) + got.astype(jnp.float32)).astype(jnp.bfloat16)
    terms = lax.all_to_all(chip_term, ("section", *CHIP), split_axis=0, concat_axis=0, tiled=True)
    kv_grad = jnp.sum(terms.astype(jnp.float32), axis=0)
    kv_grad = kv_grad.reshape(-1, PAIRS, 2, 128).transpose(0, 2, 1, 3).reshape(-1, 2 * INNER)

    context = (context_own + lax.ppermute(context_other, "section", SWAP)).astype(jnp.bfloat16)
    decoded = (source + jnp.dot(context, w_output, preferred_element_type=jnp.float32)).astype(
        jnp.bfloat16
    )
    d_query = (dq_own + lax.ppermute(dq_other, "section", SWAP)).astype(jnp.bfloat16)
    d_scaled = jnp.dot(d_query, w_query.T, preferred_element_type=jnp.float32) * caption_gain
    caption_grad = grad_out.astype(jnp.float32) + inv_rms * (
        d_scaled - source * inv_rms * inv_rms * jnp.mean(d_scaled * source, axis=-1, keepdims=True)
    )
    return (
        decoded[None, None],
        caption_grad.astype(jnp.bfloat16)[None, None],
        memory_grad,
        kv_grad,
    )


def solution(mesh):
    finer = Mesh(
        mesh.devices.reshape(mesh.shape["section"], 2, 4, 4, 2),
        ("section", "dev_0", "dev_1", "dev_2", "dev_3"),
    )
    placed = (
        P(SECTION_DEV, None, None),
        P(),
        P(),
        P(),
        P(),
        P(),
        P("section", DEV, None, None),
        P("section", DEV),
        P(),
        P(),
        P(),
        P(),
        P("section", DEV, None, None),
    )
    return jax.shard_map(
        local,
        mesh=finer,
        in_specs=placed,
        out_specs=(
            P("section", DEV, None, None),
            P("section", DEV, None, None),
            P(SECTION_DEV, None, None),
            P(SECTION_DEV, None),
        ),
        check_vma=False,
    )
```

```python
import functools

import jax
import jax.numpy as jnp
from jax import lax
from jax.experimental import pallas as pl
from jax.experimental.pallas import tpu as pltpu
from jax.sharding import Mesh
from jax.sharding import PartitionSpec as P


HEADS = 16
HEAD_DIM = 64
INNER = 1024
QDIM = 1024
QUERIES = 32
FRAMES = 32
WIN_DEV = 16
MOST_WIN = 20
CAPLEN = 128
PAIRS = HEADS // 2
ROWS = MOST_WIN * QUERIES
DEV = ("dev_0", "dev_1", "dev_2", "dev_3")
CHIP = ("dev_0", "dev_1", "dev_2")
CORE = "dev_3"
SECTION_DEV = ("section", "dev_0", "dev_1", "dev_2", "dev_3")
SWAP = [(0, 1), (1, 0)]

EPSILON = 1e-06
DEAD = -1e30


NT = (((1,), (1,)), ((), ()))
TN = (((0,), (0,)), ((), ()))
NN = (((1,), (0,)), ((), ()))


def dot(a, b, dims=NN):
    return lax.dot_general(a, b, dims, preferred_element_type=jnp.float32)


def smem():
    return pl.BlockSpec(memory_space=pltpu.SMEM)


def anywhere():
    return pl.BlockSpec(memory_space=pl.ANY)


def run_start(counts_ref, section, video):
    step = lambda v, total: total + jnp.where(v < video, counts_ref[section, v], 0)
    return lax.fori_loop(0, counts_ref.shape[1], step, jnp.int32(0))


def vmem():
    return pl.BlockSpec(memory_space=pltpu.VMEM)


def limit(mib):
    return pltpu.CompilerParams(vmem_limit_bytes=mib << 20)


def columns(pair, base=0):
    return pl.ds(pl.multiple_of(base + pair * 128, 128), 128)


CUTS = [pl.ds(512 * c, 512) for c in range(4)]


def compress_kernel(
    place_ref,
    counts_ref,
    queries_ref,
    gain_ref,
    frames_hbm,
    weight_hbm,
    out_hbm,
    sent_hbm,
    frames_ref,
    weight_ref,
    pairs_ref,
    context_ref,
    out_ref,
    memory_ref,
    slots_ref,
    fetch_sems,
    sems,
):
    copies = 4
    rows = copies * FRAMES
    wide = 2 * QUERIES * copies
    frames_fetch = pltpu.make_async_copy(frames_hbm, frames_ref, fetch_sems.at[4])
    out_fetch = pltpu.make_async_copy(out_hbm, out_ref, fetch_sems.at[5])
    fetches = [
        pltpu.make_async_copy(weight_hbm.at[:, cut], weight_ref.at[:, cut], fetch_sems.at[c])
        for c, cut in enumerate(CUTS)
    ]
    frames_fetch.start()
    for fetch in fetches:
        fetch.start()
    out_fetch.start()
    section, video_id = place_ref[0], place_ref[1]
    videos = counts_ref.shape[1]

    def owned(v, start):
        end = start + counts_ref[section, v]
        window = (start - video_id + 2 * videos - 1) // videos - 1

        @pl.when(window * videos + video_id < end)
        def _():
            slots_ref[window] = v // 2

        return end

    lax.fori_loop(0, videos, owned, jnp.int32(0))
    frames_fetch.wait()
    for fetch, cut in zip(fetches, CUTS):
        fetch.wait()
        pairs_ref[:, cut] = dot(frames_ref[...], weight_ref[:, cut]).astype(jnp.bfloat16)

    row = lax.broadcasted_iota(jnp.int32, (rows, wide), 0)
    column = lax.broadcasted_iota(jnp.int32, (rows, wide), 1)
    same = row // FRAMES == column // (2 * QUERIES)
    low = lax.broadcasted_iota(jnp.int32, (QUERIES, 128), 1) < HEAD_DIM

    @pl.loop(0, PAIRS, unroll=2)
    def _(pair):
        at = columns(pair)
        queries = queries_ref[:, at]
        zero = jnp.zeros_like(queries)
        apart = [jnp.where(low, queries, zero), jnp.where(low, zero, queries)]
        apart = jnp.concatenate(apart * copies, axis=0)
        for group in range(WIN_DEV // copies):
            inside = pl.ds(group * rows, rows)
            keys, values = pairs_ref[inside, at], pairs_ref[inside, columns(pair, QDIM)]
            scores = (dot(keys, apart, NT) * HEAD_DIM ** (-0.5)).reshape(copies, FRAMES, wide)
            grown = jnp.exp(scores - jnp.max(scores, axis=1, keepdims=True))
            attention = grown * (1.0 / jnp.sum(grown, axis=1, keepdims=True))
            attention = jnp.where(same, attention.reshape(rows, wide), 0.0).astype(jnp.bfloat16)
            product = dot(attention, values, TN)
            for c in range(copies):
                start = c * 2 * QUERIES
                mixed = jnp.where(
                    low,
                    product[start : start + QUERIES],
                    product[start + QUERIES : start + 2 * QUERIES],
                )
                window = group * copies + c
                context_ref[pl.ds(window * QUERIES, QUERIES), at] = mixed.astype(jnp.bfloat16)

    out_fetch.wait()
    base = queries_ref[...].astype(jnp.float32)
    gain = gain_ref[...]
    for group in range(WIN_DEV // copies):
        projected = dot(context_ref[pl.ds(group * rows, rows), :], out_ref[...])
        hidden = projected.reshape(copies, QUERIES, QDIM) + base[None]
        scale = lax.rsqrt(jnp.mean(hidden * hidden, axis=-1, keepdims=True) + EPSILON)
        memory_ref[pl.ds(group * copies, copies)] = (hidden * scale * gain[None]).astype(
            jnp.bfloat16
        )
        for window in range(group * copies, (group + 1) * copies):
            pltpu.make_async_copy(
                memory_ref.at[window], sent_hbm.at[slots_ref[window]], sems.at[window]
            ).start()
    for window in range(WIN_DEV):
        pltpu.make_async_copy(memory_ref.at[window], sent_hbm.at[0], sems.at[window]).wait()


def compress_windows(place, counts, frames, queries, frame_kv, query_out, gain):
    chips = counts.shape[1] // 2
    tall = WIN_DEV * FRAMES
    return pl.pallas_call(
        compress_kernel,
        out_shape=jax.ShapeDtypeStruct((chips, QUERIES, QDIM), jnp.bfloat16),
        in_specs=[smem(), smem(), vmem(), vmem(), anywhere(), anywhere(), anywhere()],
        out_specs=anywhere(),
        scratch_shapes=[
            pltpu.VMEM((tall, QDIM), jnp.bfloat16),
            pltpu.VMEM((QDIM, 2 * QDIM), jnp.bfloat16),
            pltpu.VMEM((tall, 2 * QDIM), jnp.bfloat16),
            pltpu.VMEM((tall, QDIM), jnp.bfloat16),
            pltpu.VMEM((QDIM, QDIM), jnp.bfloat16),
            pltpu.VMEM((WIN_DEV, QUERIES, QDIM), jnp.bfloat16),
            pltpu.SMEM((WIN_DEV,), jnp.int32),
            pltpu.SemaphoreType.DMA((6,)),
            pltpu.SemaphoreType.DMA((WIN_DEV,)),
        ],
        cost_estimate=pl.CostEstimate(
            flops=6 * 10**9, bytes_accessed=9 * 10**6, transcendentals=10**6
        ),
        name="compress_windows",
    )(place, counts, queries, gain[None], frames.reshape(tall, QDIM), frame_kv, query_out)


def stacked(own_ref, other_ref, at):
    both = jnp.concatenate([own_ref[:, at], other_ref[:, at]], axis=0)
    lane = lax.broadcasted_iota(jnp.int32, both.shape, 1)
    zero = jnp.zeros_like(both)
    return jnp.concatenate(
        [jnp.where(lane < HEAD_DIM, both, zero), jnp.where(lane < HEAD_DIM, zero, both)], axis=0
    )


def masked_scores(keys, queries, live):
    scores = dot(keys, queries, NT)
    row = lax.broadcasted_iota(jnp.int32, scores.shape, 0)
    return jnp.where(row < live, scores, DEAD)


def touch_kernel(place_ref, weight_ref, out_ref):
    for k in range(place_ref.shape[0]):
        out_ref[k] = place_ref[k]


def touched(place, memory_kv):
    return pl.pallas_call(
        touch_kernel,
        out_shape=jax.ShapeDtypeStruct(place.shape, place.dtype),
        in_specs=[smem(), vmem()],
        out_specs=smem(),
        compiler_params=limit(16),
        cost_estimate=pl.CostEstimate(flops=10**9, bytes_accessed=4 * 10**6, transcendentals=0),
        name="touched",
    )(place, memory_kv)


def project_kernel(
    place_ref, counts_ref, arrived_ref, beside_ref, weight_ref, half_ref, kv_ref, sems
):
    section, video_id = place_ref[0], place_ref[1]
    videos = counts_ref.shape[1]
    core = video_id % 2
    count = counts_ref[section, video_id]
    start = run_start(counts_ref, section, video_id)

    def block(p):
        return half_ref.at[pl.ds(pl.multiple_of(p * QUERIES, QUERIES), QUERIES)]

    @pl.loop(0, MOST_WIN)
    def _(p):
        rank = start + p
        slot = rank % videos // 2
        near = rank % 2 == core

        @pl.when((p < count) & near)
        def _():
            pltpu.make_async_copy(arrived_ref.at[slot], block(p), sems.at[p]).start()

        @pl.when((p < count) & jnp.logical_not(near))
        def _():
            pltpu.make_async_copy(beside_ref.at[slot], block(p), sems.at[p]).start()

        @pl.when(p >= count)
        def _():
            half_ref[pl.ds(pl.multiple_of(p * QUERIES, QUERIES), QUERIES), :] = jnp.zeros(
                (QUERIES, QDIM), jnp.bfloat16
            )

    @pl.loop(0, MOST_WIN)
    def _(p):
        @pl.when(p < count)
        def _():
            pltpu.make_async_copy(arrived_ref.at[0], block(p), sems.at[p]).wait()

    for cut in CUTS:
        kv_ref[:, cut] = dot(half_ref[...], weight_ref[:, cut]).astype(jnp.bfloat16)


def project_memory(place, counts, arrived, beside, memory_kv):
    return pl.pallas_call(
        project_kernel,
        out_shape=(
            jax.ShapeDtypeStruct((ROWS, QDIM), jnp.bfloat16),
            jax.ShapeDtypeStruct((ROWS, 2 * INNER), jnp.bfloat16),
        ),
        in_specs=[smem(), smem(), anywhere(), anywhere(), vmem()],
        out_specs=(vmem(), vmem()),
        scratch_shapes=[pltpu.SemaphoreType.DMA((MOST_WIN,))],
        compiler_params=limit(16),
        cost_estimate=pl.CostEstimate(
            flops=5 * 10**9, bytes_accessed=10**7, transcendentals=0
        ),
        name="project_memory",
    )(place, counts, arrived, beside, memory_kv)


def stats_kernel(
    place_ref, counts_ref, q_own, q_other, dc_own, dc_other, kv_ref, stats_ref
):
    live = counts_ref[place_ref[0], place_ref[1]] * QUERIES

    @pl.loop(0, PAIRS, unroll=2)
    def _(pair):
        at = columns(pair)
        keys, values = kv_ref[:, at], kv_ref[:, columns(pair, INNER)]
        scores = masked_scores(keys, stacked(q_own, q_other, at), live)
        top = jnp.max(scores, axis=0, keepdims=True)
        grown = jnp.exp(scores - top)
        d_probs = dot(values, stacked(dc_own, dc_other, at), NT)
        stats_ref[0, pl.ds(pair, 1), :] = top
        stats_ref[1, pl.ds(pair, 1), :] = jnp.sum(grown, axis=0, keepdims=True)
        stats_ref[2, pl.ds(pair, 1), :] = jnp.sum(grown * d_probs, axis=0, keepdims=True)


def attention_stats(place, counts, tokens, key_value):
    return pl.pallas_call(
        stats_kernel,
        out_shape=jax.ShapeDtypeStruct((3, PAIRS, 4 * CAPLEN), jnp.float32),
        in_specs=[smem(), smem()] + [vmem()] * 5,
        out_specs=vmem(),
        compiler_params=limit(16),
        cost_estimate=pl.CostEstimate(
            flops=5 * 10**9, bytes_accessed=4 * 10**6, transcendentals=3 * 10**6
        ),
        name="attention_stats",
    )(place, counts, *tokens, key_value)


def pack_kernel(place_ref, counts_ref, own_hbm, near_hbm, out_ref, sems):
    section, video_id = place_ref[0], place_ref[1]
    videos = counts_ref.shape[1]
    core = video_id % 2
    sibling = video_id + 1 - 2 * core
    count, count_near = counts_ref[section, video_id], counts_ref[section, sibling]
    start = run_start(counts_ref, section, video_id)
    start_near = jnp.where(core == 0, start + count, start - count_near)
    for act in ("start", "wait"):
        for source, first, size in ((own_hbm, start, count), (near_hbm, start_near, count_near)):
            odd = (core - first) % 2

            @pl.loop(0, MOST_WIN // 2)
            def _(i):
                p = odd + 2 * i
                slot = (first + p) % videos // 2

                @pl.when(p < size)
                def _():
                    copy = pltpu.make_async_copy(source.at[p], out_ref.at[slot], sems.at[slot])
                    copy.start() if act == "start" else copy.wait()


def pack_gradients(place, counts, own, near):
    chips = counts.shape[1] // 2
    return pl.pallas_call(
        pack_kernel,
        out_shape=jax.ShapeDtypeStruct((chips, QUERIES, QDIM), jnp.bfloat16),
        in_specs=[smem(), smem(), anywhere(), anywhere()],
        out_specs=pl.BlockSpec(memory_space=pltpu.VMEM),
        scratch_shapes=[pltpu.SemaphoreType.DMA((chips,))],
        cost_estimate=pl.CostEstimate(
            flops=2 * 10**9, bytes_accessed=4 * 10**6, transcendentals=0
        ),
        name="pack_gradients",
    )(place, counts, own, near)


def unpack_kernel(place_ref, counts_ref, returned_hbm, out_ref, sems):
    section, video_id = place_ref[0], place_ref[1]
    videos = counts_ref.shape[1]

    def take(v, start):
        end = start + counts_ref[section, v]
        window = (start - video_id + 2 * videos - 1) // videos - 1

        @pl.when(window * videos + video_id < end)
        def _():
            pltpu.make_async_copy(
                returned_hbm.at[v // 2], out_ref.at[window], sems.at[window]
            ).start()

        return end

    lax.fori_loop(0, videos, take, jnp.int32(0))
    for window in range(WIN_DEV):
        pltpu.make_async_copy(returned_hbm.at[0], out_ref.at[window], sems.at[window]).wait()


def unpack_gradients(place, counts, returned):
    return pl.pallas_call(
        unpack_kernel,
        out_shape=jax.ShapeDtypeStruct((WIN_DEV, QUERIES, QDIM), jnp.bfloat16),
        in_specs=[smem(), smem(), anywhere()],
        out_specs=pl.BlockSpec(memory_space=pltpu.VMEM),
        scratch_shapes=[pltpu.SemaphoreType.DMA((WIN_DEV,))],
        cost_estimate=pl.CostEstimate(
            flops=2 * 10**9, bytes_accessed=2 * 10**6, transcendentals=0
        ),
        name="unpack_gradients",
    )(place, counts, returned)


RINGS = 4
PART = QDIM // RINGS


def turn_kernel(place_ref, half_ref, kept_ref, given_ref, turned):
    core = place_ref[1] % 2
    turned[...] = half_ref[...].T
    for flip, out_ref in ((core, kept_ref), (1 - core, given_ref)):

        @pl.loop(0, RINGS)
        def _(first):
            for second in range(RINGS):
                for third in range(RINGS):
                    first_at = (place_ref[2 + flip] + first) % RINGS
                    second_at = (place_ref[3 - flip] + second) % RINGS
                    x = jnp.where(flip == 0, first_at, second_at)
                    y = jnp.where(flip == 0, second_at, first_at)
                    z = (place_ref[4] + third) % RINGS
                    chip = ((z % 2 * 2 + z // 2) * RINGS + x) * RINGS + y
                    to = (first * RINGS + second) * RINGS + third
                    out_ref[pl.ds(pl.multiple_of(to * 16, 16), 16), :] = turned[
                        pl.ds(pl.multiple_of(chip * 16, 16), 16), :
                    ]


def turned_memory(place, half):
    out = jax.ShapeDtypeStruct((QDIM, ROWS), jnp.bfloat16)
    return pl.pallas_call(
        turn_kernel,
        out_shape=(out, out),
        in_specs=[smem(), vmem()],
        out_specs=(vmem(), vmem()),
        scratch_shapes=[pltpu.VMEM((QDIM, ROWS), jnp.bfloat16)],
        compiler_params=limit(16),
        cost_estimate=pl.CostEstimate(
            flops=2 * 10**9, bytes_accessed=4 * 10**6, transcendentals=0
        ),
        name="turned_memory",
    )(place, half)


def term_kernel(sibling, place_ref, turned_ref, sum_ref, out_ref):
    core = place_ref[1] % 2
    which = 1 - core if sibling else core
    for step in range(RINGS):
        rows = pl.ds(step * PART, PART)
        out_ref[step] = dot(turned_ref[rows, :], sum_ref[which]).astype(jnp.bfloat16)


def gradient_term(place, turned, d_sum, sibling):
    return pl.pallas_call(
        functools.partial(term_kernel, sibling),
        out_shape=jax.ShapeDtypeStruct((RINGS, PART, INNER), jnp.bfloat16),
        in_specs=[smem(), vmem(), vmem()],
        out_specs=vmem(),
        compiler_params=limit(16),
        cost_estimate=pl.CostEstimate(
            flops=3 * 10**9, bytes_accessed=5 * 10**6, transcendentals=0
        ),
        name="given_term" if sibling else "kept_term",
    )(place, turned, d_sum)


def moved(shifts):
    pairs = []
    for device in range(128):
        core, y, x, z = device % 2, device // 2 % 4, device // 8 % 4, device // 64 + device // 32 % 2 * 2
        first, second, third = shifts
        along = (second, first) if core else (first, second)
        x, y, z = (x + along[0]) % RINGS, (y + along[1]) % RINGS, (z + third) % RINGS
        pairs.append((device, ((z % 2 * 2 + z // 2) * 16 + x * 4 + y) * 2 + core))
    return pairs


def shifted(value, *shifts):
    return lax.ppermute(value.astype(jnp.bfloat16), SECTION_DEV, moved(shifts))


def wider(value):
    return value.astype(jnp.float32)


def summed_terms(kept, got):
    total = [wider(kept[r]) + wider(got[r]) for r in range(RINGS)]
    half = PART // 2
    ahead = shifted(total[2][:half], 1, 0, 0)
    behind = shifted(total[2][half:], RINGS - 1, 0, 0)
    nearer = jnp.concatenate([total[1][:half] + wider(ahead), total[1][half:]], axis=0)
    farther = jnp.concatenate([total[3][:half], total[3][half:] + wider(behind)], axis=0)
    whole = (
        total[0]
        + wider(shifted(nearer, 1, 0, 0))
        + wider(shifted(farther, RINGS - 1, 0, 0))
    )
    total = whole.reshape(RINGS, -1, INNER)
    sent = [wider(shifted(total[r], 0, r, 0)) for r in range(1, RINGS)]
    total = (total[0] + sent[0] + sent[1] + sent[2]).reshape(RINGS, -1, INNER)
    return [total[0]] + [shifted(total[r], 0, 0, r) for r in range(1, RINGS)]


def heads_apart(product):
    both = 2 * CAPLEN
    rows = jnp.concatenate([product[:HEAD_DIM, :both], product[HEAD_DIM:, both:]], axis=0)
    return rows.T


def grads_kernel(
    place_ref,
    counts_ref,
    weight_ref,
    q_own,
    q_other,
    dc_own,
    dc_other,
    kv_ref,
    stats_ref,
    peer_ref,
    context_own,
    context_other,
    dq_own,
    dq_other,
    sum_ref,
    memory_ref,
):
    live = counts_ref[place_ref[0], place_ref[1]] * QUERIES

    @pl.loop(0, PAIRS)
    def _(pair):
        at = columns(pair)
        keys, values = kv_ref[:, at], kv_ref[:, columns(pair, INNER)]

        def mine(which):
            return stats_ref[which, pl.ds(pair, 1), :]

        def theirs(which):
            line = peer_ref[which, pl.ds(pair, 1), :]
            parts = [line[:, 128 * k : 128 * (k + 1)] for k in (1, 0, 3, 2)]
            return jnp.concatenate(parts, axis=1)

        top_mine, top_theirs = mine(0), theirs(0)
        top = jnp.maximum(top_mine, top_theirs)
        grow_mine, grow_theirs = jnp.exp(top_mine - top), jnp.exp(top_theirs - top)
        inverse = 1.0 / (mine(1) * grow_mine + theirs(1) * grow_theirs)
        delta = (mine(2) * grow_mine + theirs(2) * grow_theirs) * inverse

        queries, d_context = stacked(q_own, q_other, at), stacked(dc_own, dc_other, at)
        scores = masked_scores(keys, queries, live)
        probs = jnp.exp(scores - top) * inverse
        weights = probs.astype(jnp.bfloat16)
        d_probs = dot(values, d_context, NT)
        d_scores = (probs * (d_probs - delta)).astype(jnp.bfloat16)
        sum_ref[0, :, at] = dot(d_scores, queries).astype(jnp.bfloat16)
        sum_ref[1, :, at] = dot(weights, d_context).astype(jnp.bfloat16)
        context = heads_apart(dot(values, weights, TN))
        context_own[:, at] = context[:CAPLEN]
        context_other[:, at] = context[CAPLEN:].astype(jnp.bfloat16)
        d_query = heads_apart(dot(keys, d_scores, TN)) * HEAD_DIM ** (-0.5)
        dq_own[:, at] = d_query[:CAPLEN]
        dq_other[:, at] = d_query[CAPLEN:].astype(jnp.bfloat16)

    for c in range(4):
        cut = pl.ds(256 * c, 256)
        product = dot(sum_ref[0], weight_ref[cut, :INNER], NT)
        product += dot(sum_ref[1], weight_ref[cut, INNER:], NT)
        memory_ref[:, cut] = product.astype(jnp.bfloat16)


def attention_grads(place, counts, memory_kv, tokens, key_value, stats, peer):
    wide = jax.ShapeDtypeStruct((CAPLEN, INNER), jnp.float32)
    narrow = jax.ShapeDtypeStruct((CAPLEN, INNER), jnp.bfloat16)
    return pl.pallas_call(
        grads_kernel,
        out_shape=(
            wide,
            narrow,
            wide,
            narrow,
            jax.ShapeDtypeStruct((2, ROWS, INNER), jnp.bfloat16),
            jax.ShapeDtypeStruct((ROWS, QDIM), jnp.bfloat16),
        ),
        in_specs=[smem(), smem()] + [vmem()] * 8,
        out_specs=(vmem(),) * 6,
        compiler_params=limit(24),
        cost_estimate=pl.CostEstimate(
            flops=12 * 10**9, bytes_accessed=10**7, transcendentals=3 * 10**6
        ),
        name="attention_grads",
    )(place, counts, memory_kv, *tokens, key_value, stats, peer)


def local(
    frames,
    window_counts,
    learned_queries,
    frame_kv,
    query_out,
    query_gain,
    captions,
    caption_lengths,
    caption_gain,
    w_query,
    memory_kv,
    w_output,
    upstream,
):
    section = lax.axis_index("section")
    video_id = lax.axis_index(DEV)
    core = lax.axis_index(CORE)
    facts = (
        section,
        video_id,
        lax.axis_index("dev_1"),
        lax.axis_index("dev_2"),
        2 * lax.axis_index("dev_0") + section,
    )
    at = jnp.arange(8, dtype=jnp.int32)
    place = sum(jnp.where(at == k, fact, 0) for k, fact in enumerate(facts))

    sent = compress_windows(
        place, window_counts, frames, learned_queries, frame_kv, query_out, query_gain
    )
    arrived = lax.all_to_all(sent, CHIP, split_axis=0, concat_axis=0, tiled=True)
    captions, upstream, sent = lax.optimization_barrier((captions, upstream, sent))

    source = captions[0, 0].astype(jnp.float32)
    inv_rms = lax.rsqrt(jnp.mean(source * source, axis=-1, keepdims=True) + EPSILON)
    normed = (source * inv_rms * caption_gain).astype(jnp.bfloat16)
    query = jnp.dot(normed, w_query, preferred_element_type=jnp.float32).astype(jnp.bfloat16)
    query = query * jnp.bfloat16(HEAD_DIM ** (-0.5))
    row_live = jnp.arange(CAPLEN, dtype=jnp.int32) < caption_lengths[0, 0]
    grad_out = jnp.where(row_live[:, None], upstream[0, 0], jnp.zeros_like(upstream[0, 0]))
    d_context = jnp.dot(grad_out, w_output.T, preferred_element_type=jnp.float32).astype(
        jnp.bfloat16
    )
    query_other = lax.ppermute(query, "section", SWAP)
    d_context_other = lax.ppermute(d_context, "section", SWAP)

    arrived, query, d_context = lax.optimization_barrier((arrived, query, d_context))
    place = touched(place, memory_kv)
    beside = lax.ppermute(arrived, CORE, SWAP)
    tokens = (query, query_other, d_context, d_context_other)
    half, key_value = project_memory(place, window_counts, arrived, beside, memory_kv)
    stats = attention_stats(place, window_counts, tokens, key_value)
    peer = lax.ppermute(stats, "section", SWAP)
    half, stats = lax.optimization_barrier((half, stats))
    turned_kept, turned_given = turned_memory(place, half)
    peer, turned_kept, turned_given = lax.optimization_barrier((peer, turned_kept, turned_given))
    context_own, context_other, dq_own, dq_other, d_sum, d_memory = attention_grads(
        place, window_counts, memory_kv, tokens, key_value, stats, peer
    )

    d_memory = d_memory.reshape(MOST_WIN, QUERIES, QDIM)
    d_beside = lax.ppermute(d_memory, CORE, SWAP)
    given = gradient_term(place, turned_given, d_sum, True)
    got = lax.ppermute(given, CORE, SWAP)
    d_sum, given = lax.optimization_barrier((d_sum, given))
    kept = gradient_term(place, turned_kept, d_sum, False)
    d_beside, kept = lax.optimization_barrier((d_beside, kept))
    packed = pack_gradients(place, window_counts, d_memory, d_beside)
    packed, context_other, dq_other = lax.optimization_barrier((packed, context_other, dq_other))
    returned = lax.all_to_all(packed, CHIP, split_axis=0, concat_axis=0, tiled=True)
    memory_grad = unpack_gradients(place, window_counts, returned)

    context = (context_own + lax.ppermute(context_other, "section", SWAP)).astype(jnp.bfloat16)
    decoded = (source + jnp.dot(context, w_output, preferred_element_type=jnp.float32)).astype(
        jnp.bfloat16
    )
    d_query = (dq_own + lax.ppermute(dq_other, "section", SWAP)).astype(jnp.bfloat16)
    d_scaled = jnp.dot(d_query, w_query.T, preferred_element_type=jnp.float32) * caption_gain
    caption_grad = grad_out.astype(jnp.float32) + inv_rms * (
        d_scaled - source * inv_rms * inv_rms * jnp.mean(d_scaled * source, axis=-1, keepdims=True)
    )
    caption_grad = caption_grad.astype(jnp.bfloat16)

    own, *sent = summed_terms(kept, got)
    total = (own + wider(sent[0]) + wider(sent[1]) + wider(sent[2])).reshape(2, -1, INNER)
    stays = lax.dynamic_index_in_dim(total, core, 0, keepdims=False)
    leaves = lax.dynamic_index_in_dim(total, 1 - core, 0, keepdims=False)
    comes = lax.ppermute(leaves, CORE, SWAP)
    kv_grad = jnp.where(
        core == 0,
        jnp.concatenate([stays, comes], axis=1),
        jnp.concatenate([comes, stays], axis=1),
    )

    return (
        decoded[None, None],
        caption_grad[None, None],
        memory_grad,
        kv_grad,
    )


def solution(mesh):
    finer = Mesh(
        mesh.devices.reshape(mesh.shape["section"], 2, 4, 4, 2),
        ("section", "dev_0", "dev_1", "dev_2", "dev_3"),
    )
    placed = (
        P(SECTION_DEV, None, None),
        P(),
        P(),
        P(),
        P(),
        P(),
        P("section", DEV, None, None),
        P("section", DEV),
        P(),
        P(),
        P(),
        P(),
        P("section", DEV, None, None),
    )
    return jax.shard_map(
        local,
        mesh=finer,
        in_specs=placed,
        out_specs=(
            P("section", DEV, None, None),
            P("section", DEV, None, None),
            P(SECTION_DEV, None, None),
            P(SECTION_DEV, None),
        ),
        check_vma=False,
    )
```

```python
import functools

import jax
import jax.numpy as jnp
from jax import lax
from jax.experimental import pallas as pl
from jax.experimental.pallas import tpu as pltpu
from jax.sharding import Mesh
from jax.sharding import PartitionSpec as P


HEADS = 16
HEAD_DIM = 64
INNER = 1024
QDIM = 1024
QUERIES = 32
FRAMES = 32
WIN_DEV = 16
MOST_WIN = 20
CAPLEN = 128
PAIRS = HEADS // 2
ROWS = MOST_WIN * QUERIES
DEV = ("dev_0", "dev_1", "dev_2", "dev_3")
CHIP = ("dev_0", "dev_1", "dev_2")
CORE = "dev_3"
SECTION_DEV = ("section", "dev_0", "dev_1", "dev_2", "dev_3")
SWAP = [(0, 1), (1, 0)]

EPSILON = 1e-06
DEAD = -1e30


NT = (((1,), (1,)), ((), ()))
TN = (((0,), (0,)), ((), ()))
NN = (((1,), (0,)), ((), ()))


def dot(a, b, dims=NN):
    return lax.dot_general(a, b, dims, preferred_element_type=jnp.float32)


def smem():
    return pl.BlockSpec(memory_space=pltpu.SMEM)


def anywhere():
    return pl.BlockSpec(memory_space=pl.ANY)


def run_start(counts_ref, section, video):
    step = lambda v, total: total + jnp.where(v < video, counts_ref[section, v], 0)
    return lax.fori_loop(0, counts_ref.shape[1], step, jnp.int32(0))


def vmem():
    return pl.BlockSpec(memory_space=pltpu.VMEM)


def limit(mib):
    return pltpu.CompilerParams(vmem_limit_bytes=mib << 20)


def columns(pair, base=0):
    return pl.ds(pl.multiple_of(base + pair * 128, 128), 128)


CUTS = [pl.ds(512 * c, 512) for c in range(4)]


def compress_kernel(
    place_ref,
    counts_ref,
    queries_ref,
    gain_ref,
    frames_hbm,
    weight_hbm,
    out_hbm,
    sent_hbm,
    frames_ref,
    weight_ref,
    pairs_ref,
    context_ref,
    out_ref,
    memory_ref,
    slots_ref,
    fetch_sems,
    sems,
):
    copies = 4
    rows = copies * FRAMES
    wide = 2 * QUERIES * copies
    frames_fetch = pltpu.make_async_copy(frames_hbm, frames_ref, fetch_sems.at[4])
    out_fetch = pltpu.make_async_copy(out_hbm, out_ref, fetch_sems.at[5])
    fetches = [
        pltpu.make_async_copy(weight_hbm.at[:, cut], weight_ref.at[:, cut], fetch_sems.at[c])
        for c, cut in enumerate(CUTS)
    ]
    frames_fetch.start()
    for fetch in fetches:
        fetch.start()
    out_fetch.start()
    section, video_id = place_ref[0], place_ref[1]
    videos = counts_ref.shape[1]

    def owned(v, start):
        end = start + counts_ref[section, v]
        window = (start - video_id + 2 * videos - 1) // videos - 1

        @pl.when(window * videos + video_id < end)
        def _():
            slots_ref[window] = v // 2

        return end

    lax.fori_loop(0, videos, owned, jnp.int32(0))
    frames_fetch.wait()
    for fetch, cut in zip(fetches, CUTS):
        fetch.wait()
        pairs_ref[:, cut] = dot(frames_ref[...], weight_ref[:, cut]).astype(jnp.bfloat16)

    row = lax.broadcasted_iota(jnp.int32, (rows, wide), 0)
    column = lax.broadcasted_iota(jnp.int32, (rows, wide), 1)
    same = row // FRAMES == column // (2 * QUERIES)
    low = lax.broadcasted_iota(jnp.int32, (QUERIES, 128), 1) < HEAD_DIM

    @pl.loop(0, PAIRS, unroll=2)
    def _(pair):
        at = columns(pair)
        queries = queries_ref[:, at]
        zero = jnp.zeros_like(queries)
        apart = [jnp.where(low, queries, zero), jnp.where(low, zero, queries)]
        apart = jnp.concatenate(apart * copies, axis=0)
        for group in range(WIN_DEV // copies):
            inside = pl.ds(group * rows, rows)
            keys, values = pairs_ref[inside, at], pairs_ref[inside, columns(pair, QDIM)]
            scores = (dot(keys, apart, NT) * HEAD_DIM ** (-0.5)).reshape(copies, FRAMES, wide)
            grown = jnp.exp(scores - jnp.max(scores, axis=1, keepdims=True))
            attention = grown * (1.0 / jnp.sum(grown, axis=1, keepdims=True))
            attention = jnp.where(same, attention.reshape(rows, wide), 0.0).astype(jnp.bfloat16)
            product = dot(attention, values, TN)
            for c in range(copies):
                start = c * 2 * QUERIES
                mixed = jnp.where(
                    low,
                    product[start : start + QUERIES],
                    product[start + QUERIES : start + 2 * QUERIES],
                )
                window = group * copies + c
                context_ref[pl.ds(window * QUERIES, QUERIES), at] = mixed.astype(jnp.bfloat16)

    out_fetch.wait()
    base = queries_ref[...].astype(jnp.float32)
    gain = gain_ref[...]
    for group in range(WIN_DEV // copies):
        projected = dot(context_ref[pl.ds(group * rows, rows), :], out_ref[...])
        hidden = projected.reshape(copies, QUERIES, QDIM) + base[None]
        scale = lax.rsqrt(jnp.mean(hidden * hidden, axis=-1, keepdims=True) + EPSILON)
        memory_ref[pl.ds(group * copies, copies)] = (hidden * scale * gain[None]).astype(
            jnp.bfloat16
        )
        for window in range(group * copies, (group + 1) * copies):
            pltpu.make_async_copy(
                memory_ref.at[window], sent_hbm.at[slots_ref[window]], sems.at[window]
            ).start()
    for window in range(WIN_DEV):
        pltpu.make_async_copy(memory_ref.at[window], sent_hbm.at[0], sems.at[window]).wait()


def compress_windows(place, counts, frames, queries, frame_kv, query_out, gain):
    chips = counts.shape[1] // 2
    tall = WIN_DEV * FRAMES
    return pl.pallas_call(
        compress_kernel,
        out_shape=jax.ShapeDtypeStruct((chips, QUERIES, QDIM), jnp.bfloat16),
        in_specs=[smem(), smem(), vmem(), vmem(), anywhere(), anywhere(), anywhere()],
        out_specs=anywhere(),
        scratch_shapes=[
            pltpu.VMEM((tall, QDIM), jnp.bfloat16),
            pltpu.VMEM((QDIM, 2 * QDIM), jnp.bfloat16),
            pltpu.VMEM((tall, 2 * QDIM), jnp.bfloat16),
            pltpu.VMEM((tall, QDIM), jnp.bfloat16),
            pltpu.VMEM((QDIM, QDIM), jnp.bfloat16),
            pltpu.VMEM((WIN_DEV, QUERIES, QDIM), jnp.bfloat16),
            pltpu.SMEM((WIN_DEV,), jnp.int32),
            pltpu.SemaphoreType.DMA((6,)),
            pltpu.SemaphoreType.DMA((WIN_DEV,)),
        ],
        cost_estimate=pl.CostEstimate(
            flops=6 * 10**9, bytes_accessed=9 * 10**6, transcendentals=10**6
        ),
        name="compress_windows",
    )(place, counts, queries, gain[None], frames.reshape(tall, QDIM), frame_kv, query_out)


def stacked(own_ref, other_ref, at):
    both = jnp.concatenate([own_ref[:, at], other_ref[:, at]], axis=0)
    lane = lax.broadcasted_iota(jnp.int32, both.shape, 1)
    zero = jnp.zeros_like(both)
    return jnp.concatenate(
        [jnp.where(lane < HEAD_DIM, both, zero), jnp.where(lane < HEAD_DIM, zero, both)], axis=0
    )


def masked_scores(keys, queries, live):
    scores = dot(keys, queries, NT)
    row = lax.broadcasted_iota(jnp.int32, scores.shape, 0)
    return jnp.where(row < live, scores, DEAD)


def touch_kernel(place_ref, weight_ref, out_ref):
    for k in range(place_ref.shape[0]):
        out_ref[k] = place_ref[k]


def touched(place, memory_kv):
    return pl.pallas_call(
        touch_kernel,
        out_shape=jax.ShapeDtypeStruct(place.shape, place.dtype),
        in_specs=[smem(), vmem()],
        out_specs=smem(),
        compiler_params=limit(16),
        cost_estimate=pl.CostEstimate(flops=10**9, bytes_accessed=4 * 10**6, transcendentals=0),
        name="touched",
    )(place, memory_kv)


def project_kernel(
    place_ref, counts_ref, arrived_ref, beside_ref, weight_ref, half_ref, kv_ref, sems
):
    section, video_id = place_ref[0], place_ref[1]
    videos = counts_ref.shape[1]
    core = video_id % 2
    count = counts_ref[section, video_id]
    start = run_start(counts_ref, section, video_id)

    def block(p):
        return half_ref.at[pl.ds(pl.multiple_of(p * QUERIES, QUERIES), QUERIES)]

    @pl.loop(0, MOST_WIN)
    def _(p):
        rank = start + p
        slot = rank % videos // 2
        near = rank % 2 == core

        @pl.when((p < count) & near)
        def _():
            pltpu.make_async_copy(arrived_ref.at[slot], block(p), sems.at[p]).start()

        @pl.when((p < count) & jnp.logical_not(near))
        def _():
            pltpu.make_async_copy(beside_ref.at[slot], block(p), sems.at[p]).start()

        @pl.when(p >= count)
        def _():
            half_ref[pl.ds(pl.multiple_of(p * QUERIES, QUERIES), QUERIES), :] = jnp.zeros(
                (QUERIES, QDIM), jnp.bfloat16
            )

    @pl.loop(0, MOST_WIN)
    def _(p):
        @pl.when(p < count)
        def _():
            pltpu.make_async_copy(arrived_ref.at[0], block(p), sems.at[p]).wait()

    for cut in CUTS:
        kv_ref[:, cut] = dot(half_ref[...], weight_ref[:, cut]).astype(jnp.bfloat16)


def project_memory(place, counts, arrived, beside, memory_kv):
    return pl.pallas_call(
        project_kernel,
        out_shape=(
            jax.ShapeDtypeStruct((ROWS, QDIM), jnp.bfloat16),
            jax.ShapeDtypeStruct((ROWS, 2 * INNER), jnp.bfloat16),
        ),
        in_specs=[smem(), smem(), anywhere(), anywhere(), vmem()],
        out_specs=(vmem(), vmem()),
        scratch_shapes=[pltpu.SemaphoreType.DMA((MOST_WIN,))],
        compiler_params=limit(16),
        cost_estimate=pl.CostEstimate(
            flops=5 * 10**9, bytes_accessed=10**7, transcendentals=0
        ),
        name="project_memory",
    )(place, counts, arrived, beside, memory_kv)


def stats_kernel(
    place_ref, counts_ref, q_own, q_other, dc_own, dc_other, kv_ref, stats_ref
):
    live = counts_ref[place_ref[0], place_ref[1]] * QUERIES

    @pl.loop(0, PAIRS, unroll=2)
    def _(pair):
        at = columns(pair)
        keys, values = kv_ref[:, at], kv_ref[:, columns(pair, INNER)]
        scores = masked_scores(keys, stacked(q_own, q_other, at), live)
        top = jnp.max(scores, axis=0, keepdims=True)
        grown = jnp.exp(scores - top)
        d_probs = dot(values, stacked(dc_own, dc_other, at), NT)
        stats_ref[0, pl.ds(pair, 1), :] = top
        stats_ref[1, pl.ds(pair, 1), :] = jnp.sum(grown, axis=0, keepdims=True)
        stats_ref[2, pl.ds(pair, 1), :] = jnp.sum(grown * d_probs, axis=0, keepdims=True)


def attention_stats(place, counts, tokens, key_value):
    return pl.pallas_call(
        stats_kernel,
        out_shape=jax.ShapeDtypeStruct((3, PAIRS, 4 * CAPLEN), jnp.float32),
        in_specs=[smem(), smem()] + [vmem()] * 5,
        out_specs=vmem(),
        compiler_params=limit(16),
        cost_estimate=pl.CostEstimate(
            flops=5 * 10**9, bytes_accessed=4 * 10**6, transcendentals=3 * 10**6
        ),
        name="attention_stats",
    )(place, counts, *tokens, key_value)


def pack_kernel(place_ref, counts_ref, own_hbm, near_hbm, out_ref, sems):
    section, video_id = place_ref[0], place_ref[1]
    videos = counts_ref.shape[1]
    core = video_id % 2
    sibling = video_id + 1 - 2 * core
    count, count_near = counts_ref[section, video_id], counts_ref[section, sibling]
    start = run_start(counts_ref, section, video_id)
    start_near = jnp.where(core == 0, start + count, start - count_near)
    for act in ("start", "wait"):
        for source, first, size in ((own_hbm, start, count), (near_hbm, start_near, count_near)):
            odd = (core - first) % 2

            @pl.loop(0, MOST_WIN // 2)
            def _(i):
                p = odd + 2 * i
                slot = (first + p) % videos // 2

                @pl.when(p < size)
                def _():
                    copy = pltpu.make_async_copy(source.at[p], out_ref.at[slot], sems.at[slot])
                    copy.start() if act == "start" else copy.wait()


def pack_gradients(place, counts, own, near):
    chips = counts.shape[1] // 2
    return pl.pallas_call(
        pack_kernel,
        out_shape=jax.ShapeDtypeStruct((chips, QUERIES, QDIM), jnp.bfloat16),
        in_specs=[smem(), smem(), anywhere(), anywhere()],
        out_specs=pl.BlockSpec(memory_space=pltpu.VMEM),
        scratch_shapes=[pltpu.SemaphoreType.DMA((chips,))],
        cost_estimate=pl.CostEstimate(
            flops=2 * 10**9, bytes_accessed=4 * 10**6, transcendentals=0
        ),
        name="pack_gradients",
    )(place, counts, own, near)


def unpack_kernel(place_ref, counts_ref, returned_hbm, out_ref, sems):
    section, video_id = place_ref[0], place_ref[1]
    videos = counts_ref.shape[1]

    def take(v, start):
        end = start + counts_ref[section, v]
        window = (start - video_id + 2 * videos - 1) // videos - 1

        @pl.when(window * videos + video_id < end)
        def _():
            pltpu.make_async_copy(
                returned_hbm.at[v // 2], out_ref.at[window], sems.at[window]
            ).start()

        return end

    lax.fori_loop(0, videos, take, jnp.int32(0))
    for window in range(WIN_DEV):
        pltpu.make_async_copy(returned_hbm.at[0], out_ref.at[window], sems.at[window]).wait()


def unpack_gradients(place, counts, returned):
    return pl.pallas_call(
        unpack_kernel,
        out_shape=jax.ShapeDtypeStruct((WIN_DEV, QUERIES, QDIM), jnp.bfloat16),
        in_specs=[smem(), smem(), anywhere()],
        out_specs=pl.BlockSpec(memory_space=pltpu.VMEM),
        scratch_shapes=[pltpu.SemaphoreType.DMA((WIN_DEV,))],
        cost_estimate=pl.CostEstimate(
            flops=2 * 10**9, bytes_accessed=2 * 10**6, transcendentals=0
        ),
        name="unpack_gradients",
    )(place, counts, returned)


RINGS = 4
PART = QDIM // RINGS


def turn_kernel(place_ref, half_ref, kept_ref, given_ref, turned):
    core = place_ref[1] % 2
    turned[...] = half_ref[...].T
    for flip, out_ref in ((core, kept_ref), (1 - core, given_ref)):

        @pl.loop(0, RINGS)
        def _(first):
            for second in range(RINGS):
                for third in range(RINGS):
                    first_at = (place_ref[2 + flip] + first) % RINGS
                    second_at = (place_ref[3 - flip] + second) % RINGS
                    x = jnp.where(flip == 0, first_at, second_at)
                    y = jnp.where(flip == 0, second_at, first_at)
                    z = (place_ref[4] + third) % RINGS
                    chip = ((z % 2 * 2 + z // 2) * RINGS + x) * RINGS + y
                    to = (first * RINGS + second) * RINGS + third
                    out_ref[pl.ds(pl.multiple_of(to * 16, 16), 16), :] = turned[
                        pl.ds(pl.multiple_of(chip * 16, 16), 16), :
                    ]


def turned_memory(place, half):
    out = jax.ShapeDtypeStruct((QDIM, ROWS), jnp.bfloat16)
    return pl.pallas_call(
        turn_kernel,
        out_shape=(out, out),
        in_specs=[smem(), vmem()],
        out_specs=(vmem(), vmem()),
        scratch_shapes=[pltpu.VMEM((QDIM, ROWS), jnp.bfloat16)],
        compiler_params=limit(16),
        cost_estimate=pl.CostEstimate(
            flops=2 * 10**9, bytes_accessed=4 * 10**6, transcendentals=0
        ),
        name="turned_memory",
    )(place, half)


def term_kernel(sibling, place_ref, turned_ref, sum_ref, out_ref):
    core = place_ref[1] % 2
    which = 1 - core if sibling else core
    for step in range(RINGS):
        rows = pl.ds(step * PART, PART)
        out_ref[step] = dot(turned_ref[rows, :], sum_ref[which]).astype(jnp.bfloat16)


def gradient_term(place, turned, d_sum, sibling):
    return pl.pallas_call(
        functools.partial(term_kernel, sibling),
        out_shape=jax.ShapeDtypeStruct((RINGS, PART, INNER), jnp.bfloat16),
        in_specs=[smem(), vmem(), vmem()],
        out_specs=vmem(),
        compiler_params=limit(16),
        cost_estimate=pl.CostEstimate(
            flops=3 * 10**9, bytes_accessed=5 * 10**6, transcendentals=0
        ),
        name="given_term" if sibling else "kept_term",
    )(place, turned, d_sum)


def moved(shifts):
    pairs = []
    for device in range(128):
        core, y, x, z = device % 2, device // 2 % 4, device // 8 % 4, device // 64 + device // 32 % 2 * 2
        first, second, third = shifts
        along = (second, first) if core else (first, second)
        x, y, z = (x + along[0]) % RINGS, (y + along[1]) % RINGS, (z + third) % RINGS
        pairs.append((device, ((z % 2 * 2 + z // 2) * 16 + x * 4 + y) * 2 + core))
    return pairs


def shifted(value, *shifts):
    return lax.ppermute(value.astype(jnp.bfloat16), SECTION_DEV, moved(shifts))


def wider(value):
    return value.astype(jnp.float32)


def far_kernel(kept_ref, got_ref, ahead_ref, behind_ref):
    half = PART // 2
    for rows, out_ref in ((pl.ds(0, half), ahead_ref), (pl.ds(half, half), behind_ref)):
        total = wider(kept_ref[2, rows, :]) + wider(got_ref[2, rows, :])
        out_ref[...] = total.astype(jnp.bfloat16)


def near_kernel(kept_ref, got_ref, ahead_ref, behind_ref, nearer_ref, farther_ref):
    half = PART // 2
    low, high = pl.ds(0, half), pl.ds(half, half)
    for step, out_ref, more_ref, there in (
        (1, nearer_ref, ahead_ref, low),
        (3, farther_ref, behind_ref, high),
    ):
        for rows in (low, high):
            total = wider(kept_ref[step, rows, :]) + wider(got_ref[step, rows, :])
            if rows is there:
                total += wider(more_ref[...])
            out_ref[rows, :] = total.astype(jnp.bfloat16)


def own_kernel(kept_ref, got_ref, one_ref, other_ref, own_ref, *out_refs):
    size = PART // RINGS
    for step in range(RINGS):
        rows = pl.ds(step * size, size)
        total = wider(kept_ref[0, rows, :]) + wider(got_ref[0, rows, :])
        total += wider(one_ref[rows, :]) + wider(other_ref[rows, :])
        if step:
            out_refs[step - 1][...] = total.astype(jnp.bfloat16)
        else:
            own_ref[...] = total


def sums(kernel, shapes, *operands):
    return pl.pallas_call(
        kernel,
        out_shape=tuple(jax.ShapeDtypeStruct((rows, INNER), kind) for rows, kind in shapes),
        in_specs=[vmem()] * len(operands),
        out_specs=(vmem(),) * len(shapes),
        compiler_params=limit(16),
        cost_estimate=pl.CostEstimate(flops=10**9, bytes_accessed=10**6, transcendentals=0),
    )(*operands)


def summed_terms(kept, got, *done):
    narrow = jnp.bfloat16
    ahead, behind = sums(far_kernel, [(PART // 2, narrow)] * 2, kept, got)
    ahead = shifted(ahead, 1, 0, 0)
    behind = shifted(behind, RINGS - 1, 0, 0)
    nearer, farther = sums(near_kernel, [(PART, narrow)] * 2, kept, got, ahead, behind)
    sides = [shifted(nearer, 1, 0, 0), shifted(farther, RINGS - 1, 0, 0)]
    size = PART // RINGS
    total = sums(
        own_kernel, [(size, jnp.float32)] + [(size, narrow)] * (RINGS - 1), kept, got, *sides
    )
    sent = [shifted(total[r], 0, r, 0) for r in range(1, RINGS)]
    own, *done = lax.optimization_barrier((total[0], *done))
    sent = [wider(value) for value in sent]
    total = (own + sent[0] + sent[1] + sent[2]).reshape(RINGS, -1, INNER)
    return [total[0]] + [shifted(total[r], 0, 0, r) for r in range(1, RINGS)] + done


def heads_apart(product):
    both = 2 * CAPLEN
    rows = jnp.concatenate([product[:HEAD_DIM, :both], product[HEAD_DIM:, both:]], axis=0)
    return rows.T


def grads_kernel(
    place_ref,
    counts_ref,
    weight_ref,
    q_own,
    q_other,
    dc_own,
    dc_other,
    kv_ref,
    stats_ref,
    peer_ref,
    context_own,
    context_other,
    dq_own,
    dq_other,
    sum_ref,
    memory_ref,
):
    live = counts_ref[place_ref[0], place_ref[1]] * QUERIES

    @pl.loop(0, PAIRS, unroll=2)
    def _(pair):
        at = columns(pair)
        keys, values = kv_ref[:, at], kv_ref[:, columns(pair, INNER)]

        def mine(which):
            return stats_ref[which, pl.ds(pair, 1), :]

        def theirs(which):
            line = peer_ref[which, pl.ds(pair, 1), :]
            parts = [line[:, 128 * k : 128 * (k + 1)] for k in (1, 0, 3, 2)]
            return jnp.concatenate(parts, axis=1)

        top_mine, top_theirs = mine(0), theirs(0)
        top = jnp.maximum(top_mine, top_theirs)
        grow_mine, grow_theirs = jnp.exp(top_mine - top), jnp.exp(top_theirs - top)
        inverse = 1.0 / (mine(1) * grow_mine + theirs(1) * grow_theirs)
        delta = (mine(2) * grow_mine + theirs(2) * grow_theirs) * inverse

        queries, d_context = stacked(q_own, q_other, at), stacked(dc_own, dc_other, at)
        scores = masked_scores(keys, queries, live)
        probs = jnp.exp(scores - top) * inverse
        weights = probs.astype(jnp.bfloat16)
        d_probs = dot(values, d_context, NT)
        d_scores = (probs * (d_probs - delta)).astype(jnp.bfloat16)
        sum_ref[0, :, at] = dot(d_scores, queries).astype(jnp.bfloat16)
        sum_ref[1, :, at] = dot(weights, d_context).astype(jnp.bfloat16)
        context = heads_apart(dot(values, weights, TN))
        context_own[:, at] = context[:CAPLEN]
        context_other[:, at] = context[CAPLEN:].astype(jnp.bfloat16)
        d_query = heads_apart(dot(keys, d_scores, TN)) * HEAD_DIM ** (-0.5)
        dq_own[:, at] = d_query[:CAPLEN]
        dq_other[:, at] = d_query[CAPLEN:].astype(jnp.bfloat16)

    for c in range(4):
        cut = pl.ds(256 * c, 256)
        product = dot(sum_ref[0], weight_ref[cut, :INNER], NT)
        product += dot(sum_ref[1], weight_ref[cut, INNER:], NT)
        memory_ref[:, cut] = product.astype(jnp.bfloat16)


def attention_grads(place, counts, memory_kv, tokens, key_value, stats, peer):
    wide = jax.ShapeDtypeStruct((CAPLEN, INNER), jnp.float32)
    narrow = jax.ShapeDtypeStruct((CAPLEN, INNER), jnp.bfloat16)
    return pl.pallas_call(
        grads_kernel,
        out_shape=(
            wide,
            narrow,
            wide,
            narrow,
            jax.ShapeDtypeStruct((2, ROWS, INNER), jnp.bfloat16),
            jax.ShapeDtypeStruct((ROWS, QDIM), jnp.bfloat16),
        ),
        in_specs=[smem(), smem()] + [vmem()] * 8,
        out_specs=(vmem(),) * 6,
        compiler_params=limit(24),
        cost_estimate=pl.CostEstimate(
            flops=12 * 10**9, bytes_accessed=10**7, transcendentals=3 * 10**6
        ),
        name="attention_grads",
    )(place, counts, memory_kv, *tokens, key_value, stats, peer)


def local(
    frames,
    window_counts,
    learned_queries,
    frame_kv,
    query_out,
    query_gain,
    captions,
    caption_lengths,
    caption_gain,
    w_query,
    memory_kv,
    w_output,
    upstream,
):
    section = lax.axis_index("section")
    video_id = lax.axis_index(DEV)
    core = lax.axis_index(CORE)
    facts = (
        section,
        video_id,
        lax.axis_index("dev_1"),
        lax.axis_index("dev_2"),
        2 * lax.axis_index("dev_0") + section,
    )
    at = jnp.arange(8, dtype=jnp.int32)
    place = sum(jnp.where(at == k, fact, 0) for k, fact in enumerate(facts))

    sent = compress_windows(
        place, window_counts, frames, learned_queries, frame_kv, query_out, query_gain
    )
    arrived = lax.all_to_all(sent, CHIP, split_axis=0, concat_axis=0, tiled=True)
    captions, upstream, sent = lax.optimization_barrier((captions, upstream, sent))

    source = captions[0, 0].astype(jnp.float32)
    inv_rms = lax.rsqrt(jnp.mean(source * source, axis=-1, keepdims=True) + EPSILON)
    normed = (source * inv_rms * caption_gain).astype(jnp.bfloat16)
    query = jnp.dot(normed, w_query, preferred_element_type=jnp.float32).astype(jnp.bfloat16)
    query = query * jnp.bfloat16(HEAD_DIM ** (-0.5))
    row_live = jnp.arange(CAPLEN, dtype=jnp.int32) < caption_lengths[0, 0]
    grad_out = jnp.where(row_live[:, None], upstream[0, 0], jnp.zeros_like(upstream[0, 0]))
    d_context = jnp.dot(grad_out, w_output.T, preferred_element_type=jnp.float32).astype(
        jnp.bfloat16
    )
    query_other = lax.ppermute(query, "section", SWAP)
    d_context_other = lax.ppermute(d_context, "section", SWAP)

    arrived, query, d_context = lax.optimization_barrier((arrived, query, d_context))
    place = touched(place, memory_kv)
    beside = lax.ppermute(arrived, CORE, SWAP)
    tokens = (query, query_other, d_context, d_context_other)
    half, key_value = project_memory(place, window_counts, arrived, beside, memory_kv)
    stats = attention_stats(place, window_counts, tokens, key_value)
    peer = lax.ppermute(stats, "section", SWAP)
    half, stats = lax.optimization_barrier((half, stats))
    turned_kept, turned_given = turned_memory(place, half)
    peer, turned_kept, turned_given = lax.optimization_barrier((peer, turned_kept, turned_given))
    context_own, context_other, dq_own, dq_other, d_sum, d_memory = attention_grads(
        place, window_counts, memory_kv, tokens, key_value, stats, peer
    )

    d_memory = d_memory.reshape(MOST_WIN, QUERIES, QDIM)
    d_beside = lax.ppermute(d_memory, CORE, SWAP)
    given = gradient_term(place, turned_given, d_sum, True)
    got = lax.ppermute(given, CORE, SWAP)
    d_sum, given = lax.optimization_barrier((d_sum, given))
    kept = gradient_term(place, turned_kept, d_sum, False)
    packed = pack_gradients(place, window_counts, d_memory, d_beside)
    packed, context_other, dq_other = lax.optimization_barrier((packed, context_other, dq_other))
    returned = lax.all_to_all(packed, CHIP, split_axis=0, concat_axis=0, tiled=True)
    memory_grad = unpack_gradients(place, window_counts, returned)

    context = (context_own + lax.ppermute(context_other, "section", SWAP)).astype(jnp.bfloat16)
    decoded = (source + jnp.dot(context, w_output, preferred_element_type=jnp.float32)).astype(
        jnp.bfloat16
    )
    d_query = (dq_own + lax.ppermute(dq_other, "section", SWAP)).astype(jnp.bfloat16)
    d_scaled = jnp.dot(d_query, w_query.T, preferred_element_type=jnp.float32) * caption_gain
    caption_grad = grad_out.astype(jnp.float32) + inv_rms * (
        d_scaled - source * inv_rms * inv_rms * jnp.mean(d_scaled * source, axis=-1, keepdims=True)
    )
    caption_grad = caption_grad.astype(jnp.bfloat16)

    own, *sent, decoded, caption_grad = summed_terms(kept, got, decoded, caption_grad)
    total = (own + wider(sent[0]) + wider(sent[1]) + wider(sent[2])).reshape(2, -1, INNER)
    stays = lax.dynamic_index_in_dim(total, core, 0, keepdims=False)
    leaves = lax.dynamic_index_in_dim(total, 1 - core, 0, keepdims=False)
    comes = lax.ppermute(leaves, CORE, SWAP)
    kv_grad = jnp.where(
        core == 0,
        jnp.concatenate([stays, comes], axis=1),
        jnp.concatenate([comes, stays], axis=1),
    )

    return (
        decoded[None, None],
        caption_grad[None, None],
        memory_grad,
        kv_grad,
    )


def solution(mesh):
    finer = Mesh(
        mesh.devices.reshape(mesh.shape["section"], 2, 4, 4, 2),
        ("section", "dev_0", "dev_1", "dev_2", "dev_3"),
    )
    placed = (
        P(SECTION_DEV, None, None),
        P(),
        P(),
        P(),
        P(),
        P(),
        P("section", DEV, None, None),
        P("section", DEV),
        P(),
        P(),
        P(),
        P(),
        P("section", DEV, None, None),
    )
    return jax.shard_map(
        local,
        mesh=finer,
        in_specs=placed,
        out_specs=(
            P("section", DEV, None, None),
            P("section", DEV, None, None),
            P(SECTION_DEV, None, None),
            P(SECTION_DEV, None),
        ),
        check_vma=False,
    )
```

```python
import functools

import jax
import jax.numpy as jnp
from jax import lax
from jax.experimental import pallas as pl
from jax.experimental.pallas import tpu as pltpu
from jax.sharding import Mesh
from jax.sharding import PartitionSpec as P


HEADS = 16
HEAD_DIM = 64
INNER = 1024
QDIM = 1024
QUERIES = 32
FRAMES = 32
WIN_DEV = 16
MOST_WIN = 20
CAPLEN = 128
PAIRS = HEADS // 2
ROWS = MOST_WIN * QUERIES
DEV = ("dev_0", "dev_1", "dev_2", "dev_3")
CHIP = ("dev_0", "dev_1", "dev_2")
CORE = "dev_3"
SECTION_DEV = ("section", "dev_0", "dev_1", "dev_2", "dev_3")
SWAP = [(0, 1), (1, 0)]

EPSILON = 1e-06
DEAD = -1e30


NT = (((1,), (1,)), ((), ()))
TN = (((0,), (0,)), ((), ()))
NN = (((1,), (0,)), ((), ()))


def dot(a, b, dims=NN):
    return lax.dot_general(a, b, dims, preferred_element_type=jnp.float32)


def smem():
    return pl.BlockSpec(memory_space=pltpu.SMEM)


def anywhere():
    return pl.BlockSpec(memory_space=pl.ANY)


def run_start(counts_ref, section, video):
    step = lambda v, total: total + jnp.where(v < video, counts_ref[section, v], 0)
    return lax.fori_loop(0, counts_ref.shape[1], step, jnp.int32(0))


def vmem():
    return pl.BlockSpec(memory_space=pltpu.VMEM)


def limit(mib):
    return pltpu.CompilerParams(vmem_limit_bytes=mib << 20)


def columns(pair, base=0):
    return pl.ds(pl.multiple_of(base + pair * 128, 128), 128)


CUTS = [pl.ds(512 * c, 512) for c in range(4)]


def compress_kernel(
    place_ref,
    counts_ref,
    queries_ref,
    gain_ref,
    frames_hbm,
    weight_hbm,
    out_hbm,
    sent_hbm,
    frames_ref,
    weight_ref,
    pairs_ref,
    context_ref,
    out_ref,
    memory_ref,
    slots_ref,
    fetch_sems,
    sems,
):
    copies = 4
    rows = copies * FRAMES
    wide = 2 * QUERIES * copies
    frames_fetch = pltpu.make_async_copy(frames_hbm, frames_ref, fetch_sems.at[4])
    out_fetch = pltpu.make_async_copy(out_hbm, out_ref, fetch_sems.at[5])
    fetches = [
        pltpu.make_async_copy(weight_hbm.at[:, cut], weight_ref.at[:, cut], fetch_sems.at[c])
        for c, cut in enumerate(CUTS)
    ]
    frames_fetch.start()
    for fetch in fetches:
        fetch.start()
    out_fetch.start()
    section, video_id = place_ref[0], place_ref[1]
    videos = counts_ref.shape[1]

    def owned(v, start):
        end = start + counts_ref[section, v]
        window = (start - video_id + 2 * videos - 1) // videos - 1

        @pl.when(window * videos + video_id < end)
        def _():
            slots_ref[window] = v // 2

        return end

    lax.fori_loop(0, videos, owned, jnp.int32(0))
    frames_fetch.wait()
    for fetch, cut in zip(fetches, CUTS):
        fetch.wait()
        pairs_ref[:, cut] = dot(frames_ref[...], weight_ref[:, cut]).astype(jnp.bfloat16)

    row = lax.broadcasted_iota(jnp.int32, (rows, wide), 0)
    column = lax.broadcasted_iota(jnp.int32, (rows, wide), 1)
    same = row // FRAMES == column // (2 * QUERIES)
    low = lax.broadcasted_iota(jnp.int32, (QUERIES, 128), 1) < HEAD_DIM

    @pl.loop(0, PAIRS, unroll=4)
    def _(pair):
        at = columns(pair)
        queries = queries_ref[:, at]
        zero = jnp.zeros_like(queries)
        apart = [jnp.where(low, queries, zero), jnp.where(low, zero, queries)]
        apart = jnp.concatenate(apart * copies, axis=0)
        for group in range(WIN_DEV // copies):
            inside = pl.ds(group * rows, rows)
            keys, values = pairs_ref[inside, at], pairs_ref[inside, columns(pair, QDIM)]
            scores = (dot(keys, apart, NT) * HEAD_DIM ** (-0.5)).reshape(copies, FRAMES, wide)
            grown = jnp.exp(scores - jnp.max(scores, axis=1, keepdims=True))
            attention = grown * (1.0 / jnp.sum(grown, axis=1, keepdims=True))
            attention = jnp.where(same, attention.reshape(rows, wide), 0.0).astype(jnp.bfloat16)
            product = dot(attention, values, TN)
            for c in range(copies):
                start = c * 2 * QUERIES
                mixed = jnp.where(
                    low,
                    product[start : start + QUERIES],
                    product[start + QUERIES : start + 2 * QUERIES],
                )
                window = group * copies + c
                context_ref[pl.ds(window * QUERIES, QUERIES), at] = mixed.astype(jnp.bfloat16)

    out_fetch.wait()
    base = queries_ref[...].astype(jnp.float32)
    gain = gain_ref[...]
    for group in range(WIN_DEV // copies):
        projected = dot(context_ref[pl.ds(group * rows, rows), :], out_ref[...])
        hidden = projected.reshape(copies, QUERIES, QDIM) + base[None]
        scale = lax.rsqrt(jnp.mean(hidden * hidden, axis=-1, keepdims=True) + EPSILON)
        memory_ref[pl.ds(group * copies, copies)] = (hidden * scale * gain[None]).astype(
            jnp.bfloat16
        )
        for window in range(group * copies, (group + 1) * copies):
            pltpu.make_async_copy(
                memory_ref.at[window], sent_hbm.at[slots_ref[window]], sems.at[window]
            ).start()
    for window in range(WIN_DEV):
        pltpu.make_async_copy(memory_ref.at[window], sent_hbm.at[0], sems.at[window]).wait()


def compress_windows(place, counts, frames, queries, frame_kv, query_out, gain):
    chips = counts.shape[1] // 2
    tall = WIN_DEV * FRAMES
    return pl.pallas_call(
        compress_kernel,
        out_shape=jax.ShapeDtypeStruct((chips, QUERIES, QDIM), jnp.bfloat16),
        in_specs=[smem(), smem(), vmem(), vmem(), anywhere(), anywhere(), anywhere()],
        out_specs=anywhere(),
        scratch_shapes=[
            pltpu.VMEM((tall, QDIM), jnp.bfloat16),
            pltpu.VMEM((QDIM, 2 * QDIM), jnp.bfloat16),
            pltpu.VMEM((tall, 2 * QDIM), jnp.bfloat16),
            pltpu.VMEM((tall, QDIM), jnp.bfloat16),
            pltpu.VMEM((QDIM, QDIM), jnp.bfloat16),
            pltpu.VMEM((WIN_DEV, QUERIES, QDIM), jnp.bfloat16),
            pltpu.SMEM((WIN_DEV,), jnp.int32),
            pltpu.SemaphoreType.DMA((6,)),
            pltpu.SemaphoreType.DMA((WIN_DEV,)),
        ],
        cost_estimate=pl.CostEstimate(
            flops=6 * 10**9, bytes_accessed=9 * 10**6, transcendentals=10**6
        ),
        name="compress_windows",
    )(place, counts, queries, gain[None], frames.reshape(tall, QDIM), frame_kv, query_out)


def stacked(own_ref, other_ref, at):
    both = jnp.concatenate([own_ref[:, at], other_ref[:, at]], axis=0)
    lane = lax.broadcasted_iota(jnp.int32, both.shape, 1)
    zero = jnp.zeros_like(both)
    return jnp.concatenate(
        [jnp.where(lane < HEAD_DIM, both, zero), jnp.where(lane < HEAD_DIM, zero, both)], axis=0
    )


def masked_scores(keys, queries, live):
    scores = dot(keys, queries, NT)
    row = lax.broadcasted_iota(jnp.int32, scores.shape, 0)
    return jnp.where(row < live, scores, DEAD)


def touch_kernel(place_ref, weight_ref, out_ref):
    for k in range(place_ref.shape[0]):
        out_ref[k] = place_ref[k]


def touched(place, memory_kv):
    return pl.pallas_call(
        touch_kernel,
        out_shape=jax.ShapeDtypeStruct(place.shape, place.dtype),
        in_specs=[smem(), vmem()],
        out_specs=smem(),
        compiler_params=limit(16),
        cost_estimate=pl.CostEstimate(flops=10**9, bytes_accessed=4 * 10**6, transcendentals=0),
        name="touched",
    )(place, memory_kv)


def gather_kernel(place_ref, counts_ref, arrived_ref, beside_ref, half_ref, sems):
    section, video_id = place_ref[0], place_ref[1]
    videos = counts_ref.shape[1]
    core = video_id % 2
    count = counts_ref[section, video_id]
    start = run_start(counts_ref, section, video_id)

    def block(p):
        return half_ref.at[pl.ds(pl.multiple_of(p * QUERIES, QUERIES), QUERIES)]

    @pl.loop(0, MOST_WIN)
    def _(p):
        rank = start + p
        slot = rank % videos // 2
        near = rank % 2 == core

        @pl.when((p < count) & near)
        def _():
            pltpu.make_async_copy(arrived_ref.at[slot], block(p), sems.at[p]).start()

        @pl.when((p < count) & jnp.logical_not(near))
        def _():
            pltpu.make_async_copy(beside_ref.at[slot], block(p), sems.at[p]).start()

        @pl.when(p >= count)
        def _():
            half_ref[pl.ds(pl.multiple_of(p * QUERIES, QUERIES), QUERIES), :] = jnp.zeros(
                (QUERIES, QDIM), jnp.bfloat16
            )

    @pl.loop(0, MOST_WIN)
    def _(p):
        @pl.when(p < count)
        def _():
            pltpu.make_async_copy(arrived_ref.at[0], block(p), sems.at[p]).wait()


def gathered_memory(place, counts, arrived, beside):
    return pl.pallas_call(
        gather_kernel,
        out_shape=jax.ShapeDtypeStruct((ROWS, QDIM), jnp.bfloat16),
        in_specs=[smem(), smem(), anywhere(), anywhere()],
        out_specs=vmem(),
        scratch_shapes=[pltpu.SemaphoreType.DMA((MOST_WIN,))],
        compiler_params=limit(16),
        cost_estimate=pl.CostEstimate(
            flops=3 * 10**9, bytes_accessed=4 * 10**6, transcendentals=0
        ),
        name="gathered_memory",
    )(place, counts, arrived, beside)


def project_kernel(half_ref, weight_ref, kv_ref):
    for cut in CUTS:
        kv_ref[:, cut] = dot(half_ref[...], weight_ref[:, cut]).astype(jnp.bfloat16)


def project_memory(half, memory_kv):
    return pl.pallas_call(
        project_kernel,
        out_shape=jax.ShapeDtypeStruct((ROWS, 2 * INNER), jnp.bfloat16),
        in_specs=[vmem(), vmem()],
        out_specs=vmem(),
        compiler_params=limit(16),
        cost_estimate=pl.CostEstimate(
            flops=3 * 10**9, bytes_accessed=8 * 10**6, transcendentals=0
        ),
        name="project_memory",
    )(half, memory_kv)


def stats_kernel(
    place_ref, counts_ref, q_own, q_other, dc_own, dc_other, kv_ref, stats_ref
):
    live = counts_ref[place_ref[0], place_ref[1]] * QUERIES

    @pl.loop(0, PAIRS, unroll=4)
    def _(pair):
        at = columns(pair)
        keys, values = kv_ref[:, at], kv_ref[:, columns(pair, INNER)]
        scores = masked_scores(keys, stacked(q_own, q_other, at), live)
        top = jnp.max(scores, axis=0, keepdims=True)
        grown = jnp.exp(scores - top)
        d_probs = dot(values, stacked(dc_own, dc_other, at), NT)
        stats_ref[0, pl.ds(pair, 1), :] = top
        stats_ref[1, pl.ds(pair, 1), :] = jnp.sum(grown, axis=0, keepdims=True)
        stats_ref[2, pl.ds(pair, 1), :] = jnp.sum(grown * d_probs, axis=0, keepdims=True)


def attention_stats(place, counts, tokens, key_value):
    return pl.pallas_call(
        stats_kernel,
        out_shape=jax.ShapeDtypeStruct((3, PAIRS, 4 * CAPLEN), jnp.float32),
        in_specs=[smem(), smem()] + [vmem()] * 5,
        out_specs=vmem(),
        compiler_params=limit(16),
        cost_estimate=pl.CostEstimate(
            flops=5 * 10**9, bytes_accessed=4 * 10**6, transcendentals=3 * 10**6
        ),
        name="attention_stats",
    )(place, counts, *tokens, key_value)


def pack_kernel(place_ref, counts_ref, own_hbm, near_hbm, out_ref, sems):
    section, video_id = place_ref[0], place_ref[1]
    videos = counts_ref.shape[1]
    core = video_id % 2
    sibling = video_id + 1 - 2 * core
    count, count_near = counts_ref[section, video_id], counts_ref[section, sibling]
    start = run_start(counts_ref, section, video_id)
    start_near = jnp.where(core == 0, start + count, start - count_near)
    for act in ("start", "wait"):
        for source, first, size in ((own_hbm, start, count), (near_hbm, start_near, count_near)):
            odd = (core - first) % 2

            @pl.loop(0, MOST_WIN // 2)
            def _(i):
                p = odd + 2 * i
                slot = (first + p) % videos // 2

                @pl.when(p < size)
                def _():
                    copy = pltpu.make_async_copy(source.at[p], out_ref.at[slot], sems.at[slot])
                    copy.start() if act == "start" else copy.wait()


def pack_gradients(place, counts, own, near):
    chips = counts.shape[1] // 2
    return pl.pallas_call(
        pack_kernel,
        out_shape=jax.ShapeDtypeStruct((chips, QUERIES, QDIM), jnp.bfloat16),
        in_specs=[smem(), smem(), anywhere(), anywhere()],
        out_specs=pl.BlockSpec(memory_space=pltpu.VMEM),
        scratch_shapes=[pltpu.SemaphoreType.DMA((chips,))],
        cost_estimate=pl.CostEstimate(
            flops=2 * 10**9, bytes_accessed=4 * 10**6, transcendentals=0
        ),
        compiler_params=limit(24),
        name="pack_gradients",
    )(place, counts, own, near)


def unpack_kernel(place_ref, counts_ref, returned_hbm, out_ref, sems):
    section, video_id = place_ref[0], place_ref[1]
    videos = counts_ref.shape[1]

    def take(v, start):
        end = start + counts_ref[section, v]
        window = (start - video_id + 2 * videos - 1) // videos - 1

        @pl.when(window * videos + video_id < end)
        def _():
            pltpu.make_async_copy(
                returned_hbm.at[v // 2], out_ref.at[window], sems.at[window]
            ).start()

        return end

    lax.fori_loop(0, videos, take, jnp.int32(0))
    for window in range(WIN_DEV):
        pltpu.make_async_copy(returned_hbm.at[0], out_ref.at[window], sems.at[window]).wait()


def unpack_gradients(place, counts, returned):
    return pl.pallas_call(
        unpack_kernel,
        out_shape=jax.ShapeDtypeStruct((WIN_DEV, QUERIES, QDIM), jnp.bfloat16),
        in_specs=[smem(), smem(), anywhere()],
        out_specs=pl.BlockSpec(memory_space=pltpu.VMEM),
        scratch_shapes=[pltpu.SemaphoreType.DMA((WIN_DEV,))],
        cost_estimate=pl.CostEstimate(
            flops=2 * 10**9, bytes_accessed=2 * 10**6, transcendentals=0
        ),
        name="unpack_gradients",
    )(place, counts, returned)


RINGS = 4
PART = QDIM // RINGS


def turn_kernel(place_ref, half_ref, kept_ref, given_ref, turned):
    core = place_ref[1] % 2
    turned[...] = half_ref[...].T
    for flip, out_ref in ((core, kept_ref), (1 - core, given_ref)):

        @pl.loop(0, RINGS)
        def _(first):
            for second in range(RINGS):
                for third in range(RINGS):
                    first_at = (place_ref[2 + flip] + first) % RINGS
                    second_at = (place_ref[3 - flip] + second) % RINGS
                    x = jnp.where(flip == 0, first_at, second_at)
                    y = jnp.where(flip == 0, second_at, first_at)
                    z = (place_ref[4] + third) % RINGS
                    chip = ((z % 2 * 2 + z // 2) * RINGS + x) * RINGS + y
                    to = (first * RINGS + second) * RINGS + third
                    out_ref[pl.ds(pl.multiple_of(to * 16, 16), 16), :] = turned[
                        pl.ds(pl.multiple_of(chip * 16, 16), 16), :
                    ]


def turned_memory(place, half):
    out = jax.ShapeDtypeStruct((QDIM, ROWS), jnp.bfloat16)
    return pl.pallas_call(
        turn_kernel,
        out_shape=(out, out),
        in_specs=[smem(), vmem()],
        out_specs=(vmem(), vmem()),
        scratch_shapes=[pltpu.VMEM((QDIM, ROWS), jnp.bfloat16)],
        compiler_params=limit(16),
        cost_estimate=pl.CostEstimate(
            flops=2 * 10**9, bytes_accessed=4 * 10**6, transcendentals=0
        ),
        name="turned_memory",
    )(place, half)


def term_kernel(sibling, place_ref, turned_ref, sum_ref, out_ref):
    core = place_ref[1] % 2
    which = 1 - core if sibling else core
    for step in range(RINGS):
        rows = pl.ds(step * PART, PART)
        out_ref[step] = dot(turned_ref[rows, :], sum_ref[which]).astype(jnp.bfloat16)


def gradient_term(place, turned, d_sum, sibling):
    return pl.pallas_call(
        functools.partial(term_kernel, sibling),
        out_shape=jax.ShapeDtypeStruct((RINGS, PART, INNER), jnp.bfloat16),
        in_specs=[smem(), vmem(), vmem()],
        out_specs=vmem(),
        compiler_params=limit(16),
        cost_estimate=pl.CostEstimate(
            flops=3 * 10**9, bytes_accessed=5 * 10**6, transcendentals=0
        ),
        name="given_term" if sibling else "kept_term",
    )(place, turned, d_sum)


def moved(shifts):
    pairs = []
    for device in range(128):
        core, y, x, z = device % 2, device // 2 % 4, device // 8 % 4, device // 64 + device // 32 % 2 * 2
        first, second, third = shifts
        along = (second, first) if core else (first, second)
        x, y, z = (x + along[0]) % RINGS, (y + along[1]) % RINGS, (z + third) % RINGS
        pairs.append((device, ((z % 2 * 2 + z // 2) * 16 + x * 4 + y) * 2 + core))
    return pairs


def shifted(value, *shifts):
    return lax.ppermute(value.astype(jnp.bfloat16), SECTION_DEV, moved(shifts))


def wider(value):
    return value.astype(jnp.float32)


def far_kernel(kept_ref, got_ref, ahead_ref, behind_ref):
    half = PART // 2
    for rows, out_ref in ((pl.ds(0, half), ahead_ref), (pl.ds(half, half), behind_ref)):
        total = wider(kept_ref[2, rows, :]) + wider(got_ref[2, rows, :])
        out_ref[...] = total.astype(jnp.bfloat16)


def near_kernel(kept_ref, got_ref, ahead_ref, behind_ref, nearer_ref, farther_ref):
    half = PART // 2
    low, high = pl.ds(0, half), pl.ds(half, half)
    for step, out_ref, more_ref, there in (
        (1, nearer_ref, ahead_ref, low),
        (3, farther_ref, behind_ref, high),
    ):
        for rows in (low, high):
            total = wider(kept_ref[step, rows, :]) + wider(got_ref[step, rows, :])
            if rows is there:
                total += wider(more_ref[...])
            out_ref[rows, :] = total.astype(jnp.bfloat16)


def own_kernel(kept_ref, got_ref, one_ref, other_ref, own_ref, *out_refs):
    size = PART // RINGS
    for step in range(RINGS):
        rows = pl.ds(step * size, size)
        total = wider(kept_ref[0, rows, :]) + wider(got_ref[0, rows, :])
        total += wider(one_ref[rows, :]) + wider(other_ref[rows, :])
        if step:
            out_refs[step - 1][...] = total.astype(jnp.bfloat16)
        else:
            own_ref[...] = total


def sums(kernel, shapes, *operands):
    return pl.pallas_call(
        kernel,
        out_shape=tuple(jax.ShapeDtypeStruct((rows, INNER), kind) for rows, kind in shapes),
        in_specs=[vmem()] * len(operands),
        out_specs=(vmem(),) * len(shapes),
        compiler_params=limit(16),
        cost_estimate=pl.CostEstimate(flops=10**9, bytes_accessed=10**6, transcendentals=0),
    )(*operands)


def summed_terms(kept, got, *done):
    narrow = jnp.bfloat16
    ahead, behind = sums(far_kernel, [(PART // 2, narrow)] * 2, kept, got)
    ahead = shifted(ahead, 1, 0, 0)
    behind = shifted(behind, RINGS - 1, 0, 0)
    nearer, farther = sums(near_kernel, [(PART, narrow)] * 2, kept, got, ahead, behind)
    sides = [shifted(nearer, 1, 0, 0), shifted(farther, RINGS - 1, 0, 0)]
    size = PART // RINGS
    total = sums(
        own_kernel, [(size, jnp.float32)] + [(size, narrow)] * (RINGS - 1), kept, got, *sides
    )
    sent = [shifted(total[r], 0, r, 0) for r in range(1, RINGS)]
    own, *done = lax.optimization_barrier((total[0], *done))
    sent = [wider(value) for value in sent]
    total = (own + sent[0] + sent[1] + sent[2]).reshape(RINGS, -1, INNER)
    return [total[0]] + [shifted(total[r], 0, 0, r) for r in range(1, RINGS)] + done


def heads_apart(product):
    both = 2 * CAPLEN
    rows = jnp.concatenate([product[:HEAD_DIM, :both], product[HEAD_DIM:, both:]], axis=0)
    return rows.T


def grads_kernel(
    place_ref,
    counts_ref,
    weight_ref,
    q_own,
    q_other,
    dc_own,
    dc_other,
    kv_ref,
    stats_ref,
    peer_ref,
    context_own,
    context_other,
    dq_own,
    dq_other,
    sum_ref,
    memory_ref,
):
    live = counts_ref[place_ref[0], place_ref[1]] * QUERIES

    @pl.loop(0, PAIRS, unroll=2)
    def _(pair):
        at = columns(pair)
        keys, values = kv_ref[:, at], kv_ref[:, columns(pair, INNER)]

        def mine(which):
            return stats_ref[which, pl.ds(pair, 1), :]

        def theirs(which):
            line = peer_ref[which, pl.ds(pair, 1), :]
            parts = [line[:, 128 * k : 128 * (k + 1)] for k in (1, 0, 3, 2)]
            return jnp.concatenate(parts, axis=1)

        top_mine, top_theirs = mine(0), theirs(0)
        top = jnp.maximum(top_mine, top_theirs)
        grow_mine, grow_theirs = jnp.exp(top_mine - top), jnp.exp(top_theirs - top)
        inverse = 1.0 / (mine(1) * grow_mine + theirs(1) * grow_theirs)
        delta = (mine(2) * grow_mine + theirs(2) * grow_theirs) * inverse

        queries, d_context = stacked(q_own, q_other, at), stacked(dc_own, dc_other, at)
        scores = masked_scores(keys, queries, live)
        probs = jnp.exp(scores - top) * inverse
        weights = probs.astype(jnp.bfloat16)
        d_probs = dot(values, d_context, NT)
        d_scores = (probs * (d_probs - delta)).astype(jnp.bfloat16)
        sum_ref[0, :, at] = dot(d_scores, queries).astype(jnp.bfloat16)
        sum_ref[1, :, at] = dot(weights, d_context).astype(jnp.bfloat16)
        context = heads_apart(dot(values, weights, TN))
        context_own[:, at] = context[:CAPLEN]
        context_other[:, at] = context[CAPLEN:].astype(jnp.bfloat16)
        d_query = heads_apart(dot(keys, d_scores, TN)) * HEAD_DIM ** (-0.5)
        dq_own[:, at] = d_query[:CAPLEN]
        dq_other[:, at] = d_query[CAPLEN:].astype(jnp.bfloat16)

    for c in range(4):
        cut = pl.ds(256 * c, 256)
        product = dot(sum_ref[0], weight_ref[cut, :INNER], NT)
        product += dot(sum_ref[1], weight_ref[cut, INNER:], NT)
        memory_ref[:, cut] = product.astype(jnp.bfloat16)


def attention_grads(place, counts, memory_kv, tokens, key_value, stats, peer):
    wide = jax.ShapeDtypeStruct((CAPLEN, INNER), jnp.float32)
    narrow = jax.ShapeDtypeStruct((CAPLEN, INNER), jnp.bfloat16)
    return pl.pallas_call(
        grads_kernel,
        out_shape=(
            wide,
            narrow,
            wide,
            narrow,
            jax.ShapeDtypeStruct((2, ROWS, INNER), jnp.bfloat16),
            jax.ShapeDtypeStruct((ROWS, QDIM), jnp.bfloat16),
        ),
        in_specs=[smem(), smem()] + [vmem()] * 8,
        out_specs=(vmem(),) * 6,
        compiler_params=limit(24),
        cost_estimate=pl.CostEstimate(
            flops=12 * 10**9, bytes_accessed=10**7, transcendentals=3 * 10**6
        ),
        name="attention_grads",
    )(place, counts, memory_kv, *tokens, key_value, stats, peer)


def local(
    frames,
    window_counts,
    learned_queries,
    frame_kv,
    query_out,
    query_gain,
    captions,
    caption_lengths,
    caption_gain,
    w_query,
    memory_kv,
    w_output,
    upstream,
):
    section = lax.axis_index("section")
    video_id = lax.axis_index(DEV)
    core = lax.axis_index(CORE)
    facts = (
        section,
        video_id,
        lax.axis_index("dev_1"),
        lax.axis_index("dev_2"),
        2 * lax.axis_index("dev_0") + section,
    )
    at = jnp.arange(8, dtype=jnp.int32)
    place = sum(jnp.where(at == k, fact, 0) for k, fact in enumerate(facts))

    sent = compress_windows(
        place, window_counts, frames, learned_queries, frame_kv, query_out, query_gain
    )
    arrived = lax.all_to_all(sent, CHIP, split_axis=0, concat_axis=0, tiled=True)
    captions, upstream, sent = lax.optimization_barrier((captions, upstream, sent))

    source = captions[0, 0].astype(jnp.float32)
    inv_rms = lax.rsqrt(jnp.mean(source * source, axis=-1, keepdims=True) + EPSILON)
    normed = (source * inv_rms * caption_gain).astype(jnp.bfloat16)
    query = jnp.dot(normed, w_query, preferred_element_type=jnp.float32).astype(jnp.bfloat16)
    query = query * jnp.bfloat16(HEAD_DIM ** (-0.5))
    row_live = jnp.arange(CAPLEN, dtype=jnp.int32) < caption_lengths[0, 0]
    grad_out = jnp.where(row_live[:, None], upstream[0, 0], jnp.zeros_like(upstream[0, 0]))
    d_context = jnp.dot(grad_out, w_output.T, preferred_element_type=jnp.float32).astype(
        jnp.bfloat16
    )
    query_other = lax.ppermute(query, "section", SWAP)
    d_context_other = lax.ppermute(d_context, "section", SWAP)

    arrived, query, d_context = lax.optimization_barrier((arrived, query, d_context))
    place = touched(place, memory_kv)
    beside = lax.ppermute(arrived, CORE, SWAP)
    tokens = (query, query_other, d_context, d_context_other)
    half = gathered_memory(place, window_counts, arrived, beside)
    key_value = project_memory(half, memory_kv)
    stats = attention_stats(place, window_counts, tokens, key_value)
    peer = lax.ppermute(stats, "section", SWAP)
    half, stats = lax.optimization_barrier((half, stats))
    turned_kept, turned_given = turned_memory(place, half)
    peer, turned_kept, turned_given = lax.optimization_barrier((peer, turned_kept, turned_given))
    context_own, context_other, dq_own, dq_other, d_sum, d_memory = attention_grads(
        place, window_counts, memory_kv, tokens, key_value, stats, peer
    )

    d_memory = d_memory.reshape(MOST_WIN, QUERIES, QDIM)
    d_beside = lax.ppermute(d_memory, CORE, SWAP)
    given = gradient_term(place, turned_given, d_sum, True)
    got = lax.ppermute(given, CORE, SWAP)
    d_sum, given = lax.optimization_barrier((d_sum, given))
    kept = gradient_term(place, turned_kept, d_sum, False)
    packed = pack_gradients(place, window_counts, d_memory, d_beside)
    packed, context_other, dq_other = lax.optimization_barrier((packed, context_other, dq_other))
    returned = lax.all_to_all(packed, CHIP, split_axis=0, concat_axis=0, tiled=True)
    memory_grad = unpack_gradients(place, window_counts, returned)

    context = (context_own + lax.ppermute(context_other, "section", SWAP)).astype(jnp.bfloat16)
    decoded = (source + jnp.dot(context, w_output, preferred_element_type=jnp.float32)).astype(
        jnp.bfloat16
    )
    d_query = (dq_own + lax.ppermute(dq_other, "section", SWAP)).astype(jnp.bfloat16)
    d_scaled = jnp.dot(d_query, w_query.T, preferred_element_type=jnp.float32) * caption_gain
    caption_grad = grad_out.astype(jnp.float32) + inv_rms * (
        d_scaled - source * inv_rms * inv_rms * jnp.mean(d_scaled * source, axis=-1, keepdims=True)
    )
    caption_grad = caption_grad.astype(jnp.bfloat16)

    own, *sent, decoded, caption_grad = summed_terms(kept, got, decoded, caption_grad)
    total = (own + wider(sent[0]) + wider(sent[1]) + wider(sent[2])).reshape(2, -1, INNER)
    stays = lax.dynamic_index_in_dim(total, core, 0, keepdims=False)
    leaves = lax.dynamic_index_in_dim(total, 1 - core, 0, keepdims=False)
    comes = lax.ppermute(leaves, CORE, SWAP)
    kv_grad = jnp.where(
        core == 0,
        jnp.concatenate([stays, comes], axis=1),
        jnp.concatenate([comes, stays], axis=1),
    )

    return (
        decoded[None, None],
        caption_grad[None, None],
        memory_grad,
        kv_grad,
    )


def solution(mesh):
    finer = Mesh(
        mesh.devices.reshape(mesh.shape["section"], 2, 4, 4, 2),
        ("section", "dev_0", "dev_1", "dev_2", "dev_3"),
    )
    placed = (
        P(SECTION_DEV, None, None),
        P(),
        P(),
        P(),
        P(),
        P(),
        P("section", DEV, None, None),
        P("section", DEV),
        P(),
        P(),
        P(),
        P(),
        P("section", DEV, None, None),
    )
    return jax.shard_map(
        local,
        mesh=finer,
        in_specs=placed,
        out_specs=(
            P("section", DEV, None, None),
            P("section", DEV, None, None),
            P(SECTION_DEV, None, None),
            P(SECTION_DEV, None),
        ),
        check_vma=False,
    )
```
